32 devices in a mesh: row: 8 (over z, x), col: 4 (over y, core).
Axes of the slice: x: 2, y: 2, z: 4, core: 2. Of those that a mesh axis runs over, the one named last changes fastest.
Arguments:
- factor_u: float32 [1, 8, 2, 4, 512, 128], P(None, 'row', None, 'col'), may hold values from -6 to 6
- factor_v: float32 [1, 8, 2, 4, 512, 128], P(None, 'row', None, 'col'), may hold values from -6 to 6
- near_field: float32 [2, 512, 512], replicated, as said below
- sketch: float32 [2, 512, 128], replicated, may hold values from -6 to 6
- tile_ranks: int32 [3, 1, 8, 2, 4], P(None, None, None, None, 'col'), may hold values from 1 to 128, as said below
Outputs:
- out_u: float32 [1, 8, 2, 4, 512, 128], P(None, 'row', None, 'col')
- out_v: float32 [1, 8, 2, 4, 512, 128], P(None, 'row', None, 'col')
The draws below stay inside these ranges and needn't reach their ends.
Inputs may be any that keep to these rules, and one draw needn't show every extreme that they name: tile_ranks[0] is at least 16 and equals 128 on every tile (i, i); tile_ranks[1] lies between tile_ranks[0] - tile_ranks[0] // 2 and tile_ranks[0] - max(1, tile_ranks[0] // 4); tile_ranks[2] is at least 1 and at most tile_ranks[1], and when tile_ranks[1] > 1 it is at most tile_ranks[1] - max(1, tile_ranks[1] // 4). The diagonal entries of near_field[0] and near_field[1] lie between 1 and 4.
All inputs are finite; a program needn't handle non-finite values.
Results may differ from the reference program's by a relative error of at most 0.0003.
Values sent between devices are 32-bit elements; how exact they have to be, the bound alone decides.
A program may use at most 64 MiB of HBM per device.

```python
import math
import jax
import jax.numpy as jnp
from jax import lax

TILE = 512
KMAX = 128
NS_STEPS = 3
TRD = 1
TCD = 2
N_ROW = 8
N_COL = 4


def draw_near_field(key, part):
    key_diagonal, key_spread = jax.random.split(jax.random.fold_in(key, 11))
    identity = jnp.eye(TILE, dtype=jnp.float32)
    diagonal = jnp.exp(jax.random.uniform(key_diagonal, (2, TILE), jnp.float32, 0.0, 1.3862943))
    spread = jax.random.normal(key_spread, (2, TILE, TILE), jnp.float32)
    spread = spread * (0.1 / jnp.sqrt(jnp.float32(TILE)))
    diagonal = jnp.clip(diagonal, 1.0, 4.0)
    return spread * (1.0 - identity) + diagonal[:, :, None] * identity


def draw_tile_ranks(key, part):
    row_count = TRD * N_ROW
    col_count = TCD * N_COL
    label_count = max(row_count, col_count)
    key_list = jax.random.split(jax.random.fold_in(key, 29), 5)
    groups = jax.random.randint(key_list[0], (label_count,), 0, 4)
    heavy_pair = (groups[:row_count, None] == groups[None, :col_count]).astype(jnp.int32)
    base_rank = jax.random.randint(key_list[1], (row_count, col_count), KMAX // 8, KMAX // 2 + 1)
    extra_rank = jax.random.randint(key_list[2], (row_count, col_count), 0, KMAX // 2 + 1) * heavy_pair
    rank_first = jnp.minimum(base_rank + extra_rank, KMAX)
    on_diagonal = jnp.arange(row_count)[:, None] == jnp.arange(col_count)[None, :]
    rank_first = jnp.where(on_diagonal, KMAX, rank_first)
    low_first = jnp.maximum(1, rank_first // 4)
    rank_second = rank_first - jax.random.randint(key_list[3], (row_count, col_count), low_first, rank_first // 2 + 1)
    low_second = jnp.maximum(1, rank_second // 4)
    high_second = jnp.maximum(low_second, rank_second // 2)
    rank_third = jnp.maximum(1, rank_second - jax.random.randint(key_list[4], (row_count, col_count), low_second, high_second + 1))
    stacked = jnp.stack([rank_first, rank_second, rank_third]).astype(jnp.int32)
    return stacked.reshape(3, TRD, N_ROW, TCD, N_COL)


def steps_of(stream_key, shape, pieces, low, top_value):
    def one(position, blocks):
        steps = jax.random.uniform(jax.random.fold_in(jax.random.fold_in(stream_key, 6), position), (blocks,), jnp.float32, low / len(pieces), top_value / len(pieces))
        return jnp.repeat(jnp.exp(steps), shape[position] // blocks).reshape((-1,) + (1,) * (len(shape) - position - 1))

    factor_of = one(*pieces[0])
    for cut in pieces[1:]:
        factor_of = factor_of * one(*cut)
    return factor_of


def normal_values(stream_key, extent, scale, bound, cuts=(), kind=jnp.bfloat16):
    gain = steps_of(stream_key, extent, cuts, -0.22, 0.18) if cuts else 1.0
    drawn = jax.random.normal(stream_key, extent, jnp.float32) * scale * gain
    return jnp.minimum(jnp.maximum(drawn, -bound), bound).astype(kind)


def setup_inputs(seed: int = 0) -> dict:
    splits = jax.random.split(jax.random.key(seed), 6)
    factor_u = normal_values(splits[0], (TRD, N_ROW, TCD, N_COL, TILE, KMAX), 1.0, 6.0, ((1, 8), (3, 4)), jnp.float32)
    factor_v = normal_values(splits[1], (TRD, N_ROW, TCD, N_COL, TILE, KMAX), 1.0, 6.0, ((1, 8), (3, 4)), jnp.float32)
    near_field = draw_near_field(jax.random.fold_in(splits[5], 71), 0)
    sketch = normal_values(splits[3], (2, TILE, KMAX), 1.0, 6.0, (), jnp.float32)
    tile_ranks = draw_tile_ranks(jax.random.fold_in(splits[5], 71), 0)
    return {"factor_u": factor_u, "factor_v": factor_v, "near_field": near_field, "sketch": sketch, "tile_ranks": tile_ranks}


highest = lax.Precision.HIGHEST

def rank_keep(ranks, width):
    return jnp.arange(width, dtype=jnp.int32) < ranks[..., None]

def orthonormal(basis, keeper):
    gram = jnp.einsum('...tk,...tl->...kl', basis, basis, precision=highest)
    unused = 1.0 - keeper.astype(basis.dtype)
    gram = gram + jnp.eye(basis.shape[-1], dtype=basis.dtype) * unused[..., None, :]
    factor = jnp.linalg.cholesky(gram)
    solved = jax.scipy.linalg.solve_triangular(factor, jnp.swapaxes(basis, -1, -2), lower=True)
    return jnp.swapaxes(solved, -1, -2)

def recompress(full_u, full_v, sketch_block, ranks):
    root_order = math.sqrt(full_u.shape[-2])
    keeper = rank_keep(ranks, sketch_block.shape[-1])
    projected = jnp.einsum('...tq,tk->...qk', full_v, sketch_block, precision=highest)
    basis = jnp.einsum('...tq,...qk->...tk', full_u, projected, precision=highest)
    basis = basis * keeper[..., None, :].astype(basis.dtype)
    ortho = orthonormal(orthonormal(basis, keeper), keeper)
    backward = jnp.einsum('...tq,...tk->...qk', full_u, ortho, precision=highest)
    new_v = jnp.einsum('...tq,...qk->...tk', full_v, backward, precision=highest) / root_order
    return (ortho * root_order, new_v)

def update_tiles(cur_u, cur_v, low_u, low_v, up_u, up_v, sketch_block, ranks):
    far_weight = 1.0 / (8.0 * cur_u.shape[-2])
    core_block = far_weight * jnp.einsum('...tk,...tl->...kl', low_v, up_u, precision=highest)
    product_u = jnp.einsum('...tk,...kl->...tl', low_u, core_block, precision=highest)
    product_u = jnp.broadcast_to(product_u, cur_u.shape)
    full_u = jnp.concatenate([cur_u, -product_u], axis=-1)
    full_v = jnp.concatenate([cur_v, jnp.broadcast_to(up_v, cur_v.shape)], axis=-1)
    return (product_u, recompress(full_u, full_v, sketch_block, ranks))

def newton_inverse(pivot, start_inverse):
    inverse = jnp.diag(start_inverse)
    twice = 2.0 * jnp.eye(pivot.shape[0], dtype=pivot.dtype)
    for newton_step in range(NS_STEPS):
        inverse = jnp.dot(inverse, twice - jnp.dot(pivot, inverse, precision=highest), precision=highest)
    return inverse

def reference(factor_u, factor_v, near_field, sketch, tile_ranks):
    row_count = TRD * N_ROW
    col_count = TCD * N_COL
    cur_u = factor_u.reshape(row_count, col_count, TILE, KMAX)
    cur_v = factor_v.reshape(row_count, col_count, TILE, KMAX)
    all_ranks = tile_ranks.reshape(3, row_count, col_count)
    keeper = rank_keep(all_ranks[0], KMAX).astype(cur_u.dtype)[..., None, :]
    cur_u = cur_u * keeper
    cur_v = cur_v * keeper
    far_weight = 1.0 / (8.0 * TILE)
    tile_row = jnp.arange(row_count, dtype=jnp.int32)[:, None]
    tile_col = jnp.arange(col_count, dtype=jnp.int32)[None, :]
    pivot = near_field[0] + far_weight * jnp.dot(cur_u[0, 0], cur_v[0, 0].T, precision=highest)
    for panel in range(2):
        inverse = newton_inverse(pivot, 1.0 / jnp.diagonal(near_field[panel]))
        low_v = jnp.einsum('st,isk->itk', inverse, cur_v[:, panel], precision=highest)
        up_u = cur_u[panel]
        up_v = cur_v[panel]
        sketch_block = sketch[panel]

        def one_row(items):
            row_u, row_v, lead_u, lead_v, row_ranks = items
            unused_product, fresh_pair = update_tiles(row_u, row_v, lead_u[None], lead_v[None], up_u, up_v, sketch_block, row_ranks)
            return fresh_pair
        fresh_u, fresh_v = lax.map(one_row, (cur_u[panel + 1:], cur_v[panel + 1:], cur_u[panel + 1:, panel], low_v[panel + 1:], all_ranks[panel + 1, panel + 1:]))
        if panel == 0:
            core_block = far_weight * jnp.dot(low_v[1].T, cur_u[0, 1], precision=highest)
            product_one = jnp.dot(cur_u[1, 0], core_block, precision=highest)
            pivot = near_field[1] + far_weight * (jnp.dot(cur_u[1, 1], cur_v[1, 1].T, precision=highest) - jnp.dot(product_one, cur_v[0, 1].T, precision=highest))
        chosen = (tile_row > panel) & (tile_col > panel)
        if panel == 0:
            chosen = chosen & jnp.logical_not((tile_row == 1) & (tile_col == 1))
        chosen = chosen[panel + 1:, :, None, None]
        cur_u = cur_u.at[panel + 1:].set(jnp.where(chosen, fresh_u, cur_u[panel + 1:]))
        cur_v = cur_v.at[panel + 1:].set(jnp.where(chosen, fresh_v, cur_v[panel + 1:]))
        lower_here = tile_row[:, 0] > panel
        cur_v = cur_v.at[:, panel].set(jnp.where(lower_here[:, None, None], low_v, cur_v[:, panel]))
        cur_u = cur_u.at[panel, panel].set(jnp.zeros((TILE, KMAX), cur_u.dtype))
        cur_v = cur_v.at[panel, panel].set(jnp.zeros((TILE, KMAX), cur_v.dtype))
    shape_out = (TRD, N_ROW, TCD, N_COL, TILE, KMAX)
    return (cur_u.reshape(shape_out), cur_v.reshape(shape_out))
```

```python
import functools
import math

import jax
import jax.numpy as jnp
from jax import lax
from jax.experimental import pallas as pl
from jax.experimental.pallas import tpu as pltpu
from jax.sharding import PartitionSpec as P

NS_STEPS = 3
BLOCK = 16
EDGES = 5
F32 = jnp.float32
BF16 = jnp.bfloat16
MESH = pl.DeviceIdType.MESH


def split(x):
    high = x.astype(BF16)
    return high, (x - high.astype(F32)).astype(BF16)


def mm(a, b, contract_b=0):
    return lax.dot_general(a, b, (((1,), (contract_b,)), ((), ())), preferred_element_type=F32)


def stacked(a, b, contract_b=0):
    ah, al = a
    bh, bl = b
    n = ah.shape[0]
    both = mm(jnp.concatenate([ah, al], axis=0), bh, contract_b)
    return both[:n] + both[n:] + mm(ah, bl, contract_b)


def deep(a, b, contract_b=0):
    ah, al = a
    bh, bl = b
    axis = contract_b
    return mm(jnp.concatenate([ah, al], axis=1), jnp.concatenate([bh, bh], axis=axis), contract_b) + mm(
        ah, bl, contract_b
    )


def pad_rows(x, n):
    if x.shape[0] == n:
        return x
    return jnp.concatenate([x, jnp.zeros((n - x.shape[0], x.shape[1]), x.dtype)], axis=0)


def apply_inverse(high, low, scale, w, hooks):
    n = w.shape[1]
    x = scale * w
    for step in range(2**NS_STEPS - 1):
        xh, xl = split(x)
        both = mm(high[...], jnp.concatenate([xh, xl], axis=1))
        x = x + scale * (w - (both[:, :n] + both[:, n:] + mm(low[...], xh)))
        if step in hooks:
            hooks[step]()
    return x


def diagonal_inverse(near):
    n = near.shape[0]
    eye = lax.broadcasted_iota(jnp.int32, (n, n), 0) == lax.broadcasted_iota(jnp.int32, (n, n), 1)
    return 1.0 / jnp.sum(jnp.where(eye, near, 0.0), axis=1, keepdims=True)


def spread(x, j):
    return jnp.broadcast_to(x[:, j : j + 1], x.shape)


def whiten(grams, rights, order):
    count, width = len(grams), grams[0].shape[1]
    total = grams[0].shape[0]
    rest = [jnp.concatenate([g, x], axis=1) for g, x in zip(grams, rights)]
    done = [[] for _ in grams]
    start = 0
    while start < order:
        size = min(BLOCK, order - start)
        end = start + size
        tiles = size // 8
        row_id = lax.broadcasted_iota(jnp.int32, (1, 8, width), 1)
        column = lambda x, h, j: jnp.broadcast_to(x[8 * h : 8 * h + 8, start + j : start + j + 1], (8, width))
        cols = [
            [None if h < j // 8 else jnp.stack([column(x, h, j) for x in rest]) for h in range(tiles)]
            for j in range(size)
        ]
        rows = [jnp.stack([x[8 * h : 8 * h + 8] for x in rest]) for h in range(tiles)]
        lanes = rows[0].shape[2] // width
        along = lambda m: jnp.concatenate([m] * lanes, axis=2)
        scale = [jnp.ones((count, 8, width), F32) for _ in range(tiles)]
        for k in range(size):
            hk, rk = k // 8, k % 8
            lead = cols[k]
            inv = lax.rsqrt(spread(lead[hk], rk))
            inv2 = inv * inv
            masked = list(lead)
            masked[hk] = jnp.where(row_id > rk, lead[hk], 0.0)
            m = [None if x is None else x * inv2 for x in masked]
            for j in range(k + 1, size):
                hj, rj = j // 8, j % 8
                x = spread(lead[hj], rj)
                for h in range(hj, tiles):
                    step = (masked[h] * x) * inv2 if j == k + 1 else m[h] * x
                    cols[j][h] = cols[j][h] - step
            top = rows[hk][:, rk : rk + 1]
            for h in range(hk, tiles):
                rows[h] = rows[h] - along(m[h]) * top
            scale[hk] = jnp.where(row_id == rk, inv, scale[hk])
        rows = [x * along(s) for x, s in zip(rows, scale)]
        block = jnp.concatenate(rows, axis=1) if tiles > 1 else rows[0]
        for t in range(count):
            done[t].append(block[t][:, width:])
        if end < order:
            new = []
            for t in range(count):
                high = block[t].astype(BF16).astype(F32)
                low = block[t] - high
                left = [high[:, :width], low[:, :width], high[:, :width]]
                left = jnp.concatenate(left, axis=0).T[end:order].astype(BF16)
                right = jnp.concatenate([high, high, low], axis=0).astype(BF16)
                new.append(rest[t][size : order - start] - mm(left, right))
            rest = new
        start = end
    return [pad_rows(jnp.concatenate(d, axis=0), total) for d in done]


def orthonormal(bases, ranks, order, width):
    count = bases[0].shape[0]
    row = lax.broadcasted_iota(jnp.int32, (count, width), 0)
    col = lax.broadcasted_iota(jnp.int32, (count, width), 1)
    grams = []
    for basis, rank in zip(bases, ranks):
        high, low = split(basis)
        gram = stacked((high, low), (pad_rows(high, width), pad_rows(low, width)), 1)
        grams.append(gram + jnp.where((row == col) & (col >= rank), 1.0, 0.0))
    return whiten(grams, bases, order)


def basis_of(here, above, u, wide, rank):
    rows = here.shape[0]
    keep = lax.broadcasted_iota(jnp.int32, (rows, 2 * here.shape[1]), 0) < rank
    both = jnp.where(keep, jnp.concatenate([here, -above], axis=1), 0.0)
    return stacked(split(both), split(jnp.concatenate([u, wide], axis=1)), 1)


def backward(ortho, u, wide):
    back = stacked(split(ortho), split(jnp.concatenate([u, wide], axis=1)))
    width = u.shape[1]
    return jnp.concatenate([back[:, :width], -back[:, width:]], axis=1)


def new_right(back, v, up):
    width = v.shape[1]
    bh, bl = split(back)
    bh, bl = pad_rows(bh, width), pad_rows(bl, width)
    vh, vl = split(jnp.concatenate([v, up], axis=1))
    both = mm(vh, jnp.concatenate([bh, bl], axis=0), 1)
    return both[:, :width] + both[:, width:] + mm(vl, bh, 1)


class Piece:
    def __init__(self, own, ref, root, has, edges, send, recv, local=False):
        self.own, self.ref, self.root, self.has, self.edges = own, ref, root, has, edges
        self.send, self.recv, self.local = send, recv, local

    def copy(self, k, src):
        return pltpu.make_async_remote_copy(
            src_ref=src,
            dst_ref=self.ref,
            send_sem=self.send.at[k],
            recv_sem=self.recv,
            device_id=self.edges[k][1],
            device_id_type=MESH,
        )

    def send_all(self, src):
        for k, (cond, _) in enumerate(self.edges):
            @pl.when(cond)
            def _(k=k):
                self.copy(k, src).start()

    def begin(self):
        @pl.when(self.root)
        def _():
            self.send_all(self.own)
            if self.local:
                pltpu.make_async_copy(self.own, self.ref, self.recv).start()

    def forward(self, only=None):
        both = lambda cond: cond if only is None else cond & only
        if self.local:
            @pl.when(both(self.root))
            def _():
                pltpu.make_async_copy(self.ref, self.ref, self.recv).wait()

        @pl.when(both(self.has))
        def _():
            pltpu.make_async_copy(self.ref, self.ref, self.recv).wait()
            self.send_all(self.ref)

    def finish(self):
        @pl.when(self.root | self.has)
        def _():
            for k, (cond, _) in enumerate(self.edges):
                @pl.when(cond)
                def _(k=k):
                    self.copy(k, self.ref).wait_send()


def greet_all(n_row, n_col, r, c):
    barrier = pltpu.get_barrier_semaphore()
    for d in range(1, n_row):
        pl.semaphore_signal(barrier, inc=1, device_id=((r + d) % n_row, c), device_id_type=MESH)
    for d in range(1, n_col):
        pl.semaphore_signal(barrier, inc=1, device_id=(r, (c + d) % n_col), device_id_type=MESH)
    pl.semaphore_wait(barrier, n_row + n_col - 2)


def part(ref, lead, k, count):
    view = ref if lead is None else ref.at[lead]
    rows = view.shape[0] // count
    return view.at[pl.ds(k * rows, rows)]


def kernel(n_row, n_col, order_1, order_2, ranks, hu, hv, hnear, hsketch, out_u, out_v, *scratch):
    (
        u, v, near, sk, near_t, high, low, p_u, p_v, low_u, low_v, up_u, up_v, above_own, above,
        ex_u, ex_v, ex_w, wide, lower, u1, v1, u1t_own, above1_own, up1t, up1_v, above1,
        low1_u, low1_own, low1_t, send, recv, load,
    ) = scratch
    r, c = lax.axis_index("row"), lax.axis_index("col")
    height, width = u.shape[1:]
    far = 1.0 / (8.0 * height)
    rows_1, rows_2 = above.shape[1], above1.shape[1]
    two = range(2)
    level, side, levels = r // 2, r % 2, n_row // 2
    parity = c % 2
    pieces = []

    def piece(own, ref, root, has, edges, local=False):
        k = len(pieces)
        pieces.append(Piece(own, ref, root, has, edges, send.at[k], recv.at[k], local))
        return pieces[-1]

    other_row, other_col = r + 1 - 2 * side, c + 1 - 2 * parity
    spine = side == parity
    down_on = spine & (level + 1 < levels), (r + 2, c)
    down_over = spine & (level >= 1), (other_row, c)
    down_first = r == 0, (1, c)
    if levels > 1:
        beside = [
            ((r == 0) & (parity == 1), (1, c)),
            ((parity == 0) & (level == 1) & (side == 1), (r - 2, c)),
        ]
    else:
        beside = [down_first]

    def only(cond, edges):
        return [(a & cond, d) for a, d in edges]

    def down(own, ref, when):
        return piece(own, ref, (r == 0) & when, (r > 0) & when, only(when, [down_on, down_over] + beside))

    def down_1(own, ref, on, when):
        at = side == on
        edges = [
            ((r == 1) & (on == 0), (0, c)),
            (at & (level + 1 < levels), (r + 2, c)),
            (at & (level >= 1), (other_row, c)),
        ]
        return piece(own, ref, (r == 1) & when, ((r > 1) | ((r == 0) & (on == 0))) & when, only(when, edges))

    def across(own, ref, source, when):
        at = parity == source % 2
        edges = [(at, (r, other_col)), (at & (c // 2 + 1 < n_col // 2), (r, c + 2))]
        return piece(own, ref, (c == source) & when, (c != source) & when, only(when, edges), True)

    def pivot(own, ref, k):
        mine = parity == k
        edges = only(mine, [down_first, ((r == 0) & (c + 2 < n_col), (0, c + 2)), down_on, down_over])
        edges.append((mine & (r > 0), (r, other_col)))
        root = (r == 0) & (c == 0)
        if k == 1:
            edges[1] = edges[1][0] | root, (0, jnp.where(root, 1, c + 2))
            edges[0] = edges[0][0] & jnp.logical_not(root), edges[0][1]
        has = jnp.where(mine, jnp.logical_not(root), r > 0)
        return piece(own, ref, root, has, edges)

    quarters, later_rows, always = range(4), r > 1, r >= 0
    pivots = [[pivot(part(a, 0, h, 4), part(b, None, h, 4), k) for h in quarters] for k, a, b in ((0, u, p_u), (1, v, p_v))]
    lows_v = [across(part(v, 0, h, 2), part(low_v, None, h, 2), 0, r > 0) for h in two]
    lows_u = [across(part(u, 0, h, 2), part(low_u, None, h, 2), 0, r > 0) for h in two]
    ups_u = [[down(part(u, t, h, 4), part(up_u, t, h, 4), c > 0 if t == 0 else always) for h in quarters] for t in two]
    ups_a = [down(above_own, above, always)]
    ups_v = [down(part(v, t, h, 2), part(up_v, t, h, 2), c > 0 if t == 0 else always) for t in two for h in two]
    extras = [down_1(a, b, 0, c == 1) for a, b in ((u.at[0], ex_u), (v.at[0], ex_v))]
    extra_w = [down_1(wide.at[0], ex_w, 0, c == 1)]
    chains_u = [
        down_1(part(u1t_own, t, h, 4), up1t.at[t].at[pl.ds(h * (rows_1 // 4), rows_1 // 4)], parity, c > 1 if t == 0 else always)
        for t in two
        for h in quarters
    ]
    chains_a = [down_1(above1_own, above1, parity, always)]
    chains_v = [down_1(part(v1, t, h, 2), part(up1_v, t, h, 2), parity, c > 1 if t == 0 else always) for t in two for h in two]
    lows1_u = [across(part(u1, 0, h, 2), part(low1_u, None, h, 2), 1, later_rows) for h in two]
    lows1_t = [across(part(low1_own, None, h, 2), part(low1_t, None, h, 2), 1, later_rows) for h in two]

    def begin(*groups):
        for g in groups:
            for x in g:
                x.begin()

    def forward(*groups, only=None):
        for g in groups:
            for x in g:
                x.forward(only)

    loads = [(hu, u), (hv, v), (hsketch, sk), (hnear, near)]
    copies = [pltpu.make_async_copy(a, b, load.at[k]) for k, (a, b) in enumerate(loads)]
    for x in copies:
        x.start()
    greet_all(n_row, n_col, r, c)
    for x in copies[:3]:
        x.wait()
    col_id = lax.broadcasted_iota(jnp.int32, (height, width), 1)
    for t in two:
        keep = col_id < ranks[0, 0, t, 0, r]
        u[t] = jnp.where(keep, u[t], 0.0)
        v[t] = jnp.where(keep, v[t], 0.0)
    begin(pivots[1], pivots[0], lows_v, lows_u, extras)
    sketch_t = [split(sk[k].T[:rows]) for k, rows in ((0, rows_1), (1, rows_2))]

    def here_of(v, k):
        both = stacked(sketch_t[k], split(jnp.concatenate([v[0], v[1]], axis=1)))
        return both[:, :width], both[:, width:]

    @pl.when(r == 0)
    def _():
        forward(pivots[0], pivots[1])
        begin(ups_u[0], ups_u[1])
        a, b = here_of(v, 0)
        above_own[0] = a
        above_own[1] = b
        begin(ups_a, ups_v)
        copies[3].wait()
        for t in two:
            stays = (c > 0) | (t > 0)
            out_u[t] = jnp.where(stays, u[t], 0.0)
            out_v[t] = jnp.where(stays, v[t], 0.0)
        forward(extras, extra_w, chains_u, chains_a, chains_v)

    @pl.when((r > 0) & (c == 0))
    def _():
        up_u[0] = jnp.zeros((height, width), F32)
        up_v[0] = jnp.zeros((height, width), F32)

    @pl.when(r > 0)
    def _():
        for t in two:
            up1t[t, rows_1:] = jnp.zeros((width - rows_1, height), F32)

        @pl.when(c < 2)
        def _():
            up1t[0, :rows_1] = jnp.zeros((rows_1, height), F32)
            up1_v[0] = jnp.zeros((height, width), F32)

        copies[3].wait()
        near_t[0] = near[0].T

        @pl.when((c == 1) & later_rows)
        def _():
            near_t[1] = near[1].T

        scale = diagonal_inverse(near[0])
        here = here_of(v, 0)
        for k in two:
            forward(pivots[k], only=parity == k)
        forward(extras, only=later_rows & (side == 0))
        forward(ups_u[0], ups_u[1], only=later_rows)
        forward(lows_v, lows_u)
        for k in two:
            forward(pivots[k], only=parity != k)
        pivot_t = near_t[0] + far * deep(split(p_v[...]), split(p_u[...]), 1)
        high[...], low[...] = split(pivot_t)
        ups = ups_u[0] + ups_u[1]
        hooks = {k: lambda k=k: forward(ups[k : k + 1], only=(r == 1) & (parity == 1)) for k in range(7)}
        hooks[7] = lambda: forward(ups[7:], only=(r == 1) & (parity == 1))
        lower[...] = apply_inverse(high, low, scale, low_v[...], hooks)
        hooks[7]()
        forward(ups, only=(r == 1) & (parity == 0))
        forward(extras, only=later_rows & (side == 1))
        forward(ups_a, ups_v[:1])
        core = far * stacked(
            split(lower[...].T), split(jnp.concatenate([up_u[0], up_u[1]], axis=1))
        )
        lane = lax.broadcasted_iota(jnp.int32, core.shape, 1)
        live = (lane < ranks[0, 0, 0, 0, 0]) | ((lane >= width) & (lane < width + ranks[0, 0, 1, 0, 0]))
        core = jnp.where(live, core, 0.0)
        both = deep(split(low_u[...]), split(core))
        wide[0] = both[:, :width]
        wide[1] = both[:, width:]
        begin(extra_w)
        forward(ups_v[1:2])
        rank_1 = [ranks[1, 0, t, 0, r] for t in two]
        bases = [basis_of(here[t], above[t], u[t], wide[t], rank_1[t]) for t in two]
        bases = orthonormal(bases, rank_1, order_1, width)
        forward(ups_v[2:])
        forward(extra_w, only=later_rows)
        orthos = orthonormal(bases, rank_1, order_1, width)
        root_order = math.sqrt(height)
        tile_col = [t * n_col + c for t in two]
        chosen = [(tile_col[t] > 0) & jnp.logical_not((r == 1) & (tile_col[t] == 1)) for t in two]
        for t in two:
            u1t_own[t] = orthos[t] * root_order
        begin(chains_u)
        for t in two:
            u1[t] = jnp.where(chosen[t], pad_rows(orthos[t] * root_order, width).T, u[t])
        begin(lows1_u)
        for t in two:
            right = new_right(backward(orthos[t], u[t], wide[t]), v[t], up_v[t]) * (1.0 / root_order)
            v1[t] = jnp.where(chosen[t], right, jnp.where(tile_col[t] == 0, lower[...], v[t]))
        here = here_of(v1, 1)
        above1_own[0] = here[0]
        above1_own[1] = here[1]
        begin(chains_a, chains_v)

        @pl.when(r == 1)
        def _():
            for t in two:
                stays = tile_col[t] != 1
                out_u[t] = jnp.where(stays, u1[t], 0.0)
                out_v[t] = jnp.where(stays, v1[t], 0.0)

        @pl.when(later_rows)
        def _():
            @pl.when(c == 1)
            def _():
                left = jnp.concatenate([ex_v[...], up_v[0]], axis=1)
                right = jnp.concatenate([ex_u[...], -ex_w[...]], axis=1)
                lh, ll = split(left)
                rh, rl = split(right)
                pivot_t = near_t[1] + far * (mm(lh, rh, 1) + (mm(lh, rl, 1) + mm(ll, rh, 1)))
                high[...], low[...] = split(pivot_t)
                lower[...] = apply_inverse(high, low, diagonal_inverse(near[1]), v1[0], {})
                low1_own[...] = lower[...].T[:rows_1]

            begin(lows1_t)
            forward(chains_u, lows1_u, chains_a, lows1_t)
            core = far * stacked(split(low1_t[...]), split(up1t[...].reshape(2 * width, height)), 1)
            both = deep(split(low1_u[...]), split(pad_rows(core, width)))
            wide[0] = both[:, :width]
            wide[1] = both[:, width:]
            rank_2 = [ranks[2, 0, t, 0, r] for t in two]
            bases = [basis_of(here[t], above1[t], u1[t], wide[t], rank_2[t]) for t in two]
            bases = orthonormal(bases, rank_2, order_2, width)
            forward(chains_v[:2])
            orthos = orthonormal(bases, rank_2, order_2, width)
            forward(chains_v[2:])
            for t in two:
                live = tile_col[t] > 1
                right = new_right(backward(orthos[t], u1[t], wide[t]), v1[t], up1_v[t]) * (1.0 / root_order)
                out_u[t] = jnp.where(live, pad_rows(orthos[t] * root_order, width).T, u1[t])
                out_v[t] = jnp.where(live, right, jnp.where(tile_col[t] == 1, lower[...], v1[t]))

    for x in pieces:
        x.finish()


def body(n_row, n_col, factor_u, factor_v, near_field, sketch, tile_ranks):
    tiles, height, width = factor_u.shape[2], factor_u.shape[4], factor_u.shape[5]
    u = factor_u.reshape(tiles, height, width)
    v = factor_v.reshape(tiles, height, width)
    ranks = jnp.transpose(tile_ranks, (0, 1, 3, 4, 2))
    pair, one = (tiles, height, width), (height, width)
    order_1 = width - max(1, width // 4)
    order_2 = order_1 - max(1, order_1 // 4)
    rows_1, rows_2 = -(-order_1 // 16) * 16, -(-order_2 // 16) * 16
    square = (height, height)
    f32 = lambda *shape: pltpu.VMEM(shape, F32)
    buffers = [f32(*s) for s in (pair, pair, (2,) + square, (2,) + one, (2,) + square)]
    buffers += [pltpu.VMEM(square, BF16)] * 2
    buffers += [f32(*s) for s in (one, one, one, one, pair, pair, (2, rows_1, width), (2, rows_1, width))]
    buffers += [f32(*s) for s in (one, one, one, pair, one, pair, pair, (2, rows_1, height), (2, rows_2, width))]
    buffers += [f32(*s) for s in ((2, width, height), pair, (2, rows_2, width), one, (rows_1, height), (rows_1, height))]
    pieces = 45
    any_spec = pl.BlockSpec(memory_space=pl.ANY)
    out_u, out_v = pl.pallas_call(
        functools.partial(kernel, n_row, n_col, order_1, order_2),
        out_shape=[jax.ShapeDtypeStruct(pair, F32)] * 2,
        in_specs=[pl.BlockSpec(memory_space=pltpu.SMEM)] + [any_spec] * 4,
        out_specs=[pl.BlockSpec(memory_space=pltpu.VMEM)] * 2,
        scratch_shapes=buffers
        + [
            pltpu.SemaphoreType.DMA((pieces, EDGES)),
            pltpu.SemaphoreType.DMA((pieces,)),
            pltpu.SemaphoreType.DMA((4,)),
        ],
        compiler_params=pltpu.CompilerParams(
            collective_id=0, has_side_effects=True, vmem_limit_bytes=60 * 1024 * 1024
        ),
    )(ranks, u, v, near_field, sketch)
    shape_out = (1, 1, tiles, 1, height, width)
    return (out_u.reshape(shape_out), out_v.reshape(shape_out))


def solution(mesh):
    tile_spec = P(None, "row", None, "col", None, None)
    return jax.shard_map(
        functools.partial(body, mesh.shape["row"], mesh.shape["col"]),
        mesh=mesh,
        in_specs=(tile_spec, tile_spec, P(), P(), P(None, None, None, None, "col")),
        out_specs=(tile_spec, tile_spec),
        check_vma=False,
    )
```

```python
import functools
import math

import jax
import jax.numpy as jnp
from jax import lax
from jax.experimental import pallas as pl
from jax.experimental.pallas import tpu as pltpu
from jax.sharding import PartitionSpec as P

NS_STEPS = 3
BLOCK = 16
EDGES = 5
F32 = jnp.float32
BF16 = jnp.bfloat16
MESH = pl.DeviceIdType.MESH


def split(x):
    high = x.astype(BF16)
    return high, (x - high.astype(F32)).astype(BF16)


def mm(a, b, contract_b=0):
    return lax.dot_general(a, b, (((1,), (contract_b,)), ((), ())), preferred_element_type=F32)


def stacked(a, b, contract_b=0):
    ah, al = a
    bh, bl = b
    n = ah.shape[0]
    both = mm(jnp.concatenate([ah, al], axis=0), bh, contract_b)
    return both[:n] + both[n:] + mm(ah, bl, contract_b)


def deep(a, b, contract_b=0):
    ah, al = a
    bh, bl = b
    axis = contract_b
    return mm(jnp.concatenate([ah, al], axis=1), jnp.concatenate([bh, bh], axis=axis), contract_b) + mm(
        ah, bl, contract_b
    )


def pad_rows(x, n):
    if x.shape[0] == n:
        return x
    return jnp.concatenate([x, jnp.zeros((n - x.shape[0], x.shape[1]), x.dtype)], axis=0)


def apply_inverse(high, low, scale, w, hooks):
    n = w.shape[1]
    x = scale * w
    for step in range(2**NS_STEPS - 1):
        xh, xl = split(x)
        both = mm(high[...], jnp.concatenate([xh, xl], axis=1))
        x = x + scale * (w - (both[:, :n] + both[:, n:] + mm(low[...], xh)))
        if step in hooks:
            hooks[step]()
    return x


def diagonal_inverse(near):
    n = near.shape[0]
    eye = lax.broadcasted_iota(jnp.int32, (n, n), 0) == lax.broadcasted_iota(jnp.int32, (n, n), 1)
    return 1.0 / jnp.sum(jnp.where(eye, near, 0.0), axis=1, keepdims=True)


def spread(x, j):
    return jnp.broadcast_to(x[:, j : j + 1], x.shape)


def whiten(grams, rights, order):
    count, width = len(grams), grams[0].shape[1]
    total = grams[0].shape[0]
    rest = [jnp.concatenate([g, x], axis=1) for g, x in zip(grams, rights)]
    done = [[] for _ in grams]
    start = 0
    while start < order:
        size = min(BLOCK, order - start)
        end = start + size
        tiles = size // 8
        row_id = lax.broadcasted_iota(jnp.int32, (1, 8, width), 1)
        column = lambda x, h, j: jnp.broadcast_to(x[8 * h : 8 * h + 8, start + j : start + j + 1], (8, width))
        cols = [
            [None if h < j // 8 else jnp.stack([column(x, h, j) for x in rest]) for h in range(tiles)]
            for j in range(size)
        ]
        rows = [jnp.stack([x[8 * h : 8 * h + 8] for x in rest]) for h in range(tiles)]
        lanes = rows[0].shape[2] // width
        along = lambda m: jnp.concatenate([m] * lanes, axis=2)
        scale = [jnp.ones((count, 8, width), F32) for _ in range(tiles)]
        for k in range(size):
            hk, rk = k // 8, k % 8
            lead = cols[k]
            inv = lax.rsqrt(spread(lead[hk], rk))
            inv2 = inv * inv
            masked = list(lead)
            masked[hk] = jnp.where(row_id > rk, lead[hk], 0.0)
            m = [None if x is None else x * inv2 for x in masked]
            for j in range(k + 1, size):
                hj, rj = j // 8, j % 8
                x = spread(lead[hj], rj)
                for h in range(hj, tiles):
                    step = (masked[h] * x) * inv2 if j == k + 1 else m[h] * x
                    cols[j][h] = cols[j][h] - step
            top = rows[hk][:, rk : rk + 1]
            for h in range(hk, tiles):
                rows[h] = rows[h] - along(m[h]) * top
            scale[hk] = jnp.where(row_id == rk, inv, scale[hk])
        rows = [x * along(s) for x, s in zip(rows, scale)]
        block = jnp.concatenate(rows, axis=1) if tiles > 1 else rows[0]
        for t in range(count):
            done[t].append(block[t][:, width:])
        if end < order:
            new = []
            for t in range(count):
                high = block[t].astype(BF16).astype(F32)
                low = block[t] - high
                left = [high[:, :width], low[:, :width], high[:, :width]]
                left = jnp.concatenate(left, axis=0).T[end:order].astype(BF16)
                right = jnp.concatenate([high, high, low], axis=0).astype(BF16)
                new.append(rest[t][size : order - start] - mm(left, right))
            rest = new
        start = end
    return [pad_rows(jnp.concatenate(d, axis=0), total) for d in done]


def orthonormal(bases, ranks, order, width):
    count = bases[0].shape[0]
    row = lax.broadcasted_iota(jnp.int32, (count, width), 0)
    col = lax.broadcasted_iota(jnp.int32, (count, width), 1)
    grams = []
    for basis, rank in zip(bases, ranks):
        high, low = split(basis)
        gram = stacked((high, low), (pad_rows(high, width), pad_rows(low, width)), 1)
        grams.append(gram + jnp.where((row == col) & (col >= rank), 1.0, 0.0))
    return whiten(grams, bases, order)


def basis_of(here, above, u, wide, rank):
    rows = here.shape[0]
    keep = lax.broadcasted_iota(jnp.int32, (rows, 2 * here.shape[1]), 0) < rank
    both = jnp.where(keep, jnp.concatenate([here, -above], axis=1), 0.0)
    return stacked(split(both), split(jnp.concatenate([u, wide], axis=1)), 1)


def backward(ortho, u, wide):
    back = stacked(split(ortho), split(jnp.concatenate([u, wide], axis=1)))
    width = u.shape[1]
    return jnp.concatenate([back[:, :width], -back[:, width:]], axis=1)


def new_right(back, v, up):
    width = v.shape[1]
    bh, bl = split(back)
    bh, bl = pad_rows(bh, width), pad_rows(bl, width)
    vh, vl = split(jnp.concatenate([v, up], axis=1))
    both = mm(vh, jnp.concatenate([bh, bl], axis=0), 1)
    return both[:, :width] + both[:, width:] + mm(vl, bh, 1)


class Piece:
    def __init__(self, own, ref, root, has, edges, send, recv, local=False):
        self.own, self.ref, self.root, self.has, self.edges = own, ref, root, has, edges
        self.send, self.recv, self.local = send, recv, local

    def copy(self, k, src):
        return pltpu.make_async_remote_copy(
            src_ref=src,
            dst_ref=self.ref,
            send_sem=self.send.at[k],
            recv_sem=self.recv,
            device_id=self.edges[k][1],
            device_id_type=MESH,
        )

    def send_all(self, src):
        for k, (cond, _) in enumerate(self.edges):
            @pl.when(cond)
            def _(k=k):
                self.copy(k, src).start()

    def begin(self, only=None):
        @pl.when(self.root if only is None else self.root & only)
        def _():
            self.send_all(self.own)
            if self.local:
                pltpu.make_async_copy(self.own, self.ref, self.recv).start()

    def forward(self, only=None):
        both = lambda cond: cond if only is None else cond & only
        if self.local:
            @pl.when(both(self.root))
            def _():
                pltpu.make_async_copy(self.ref, self.ref, self.recv).wait()

        @pl.when(both(self.has))
        def _():
            pltpu.make_async_copy(self.ref, self.ref, self.recv).wait()
            self.send_all(self.ref)

    def finish(self):
        @pl.when(self.root | self.has)
        def _():
            for k, (cond, _) in enumerate(self.edges):
                @pl.when(cond)
                def _(k=k):
                    self.copy(k, self.ref).wait_send()


def greet_all(n_row, n_col, r, c):
    barrier = pltpu.get_barrier_semaphore()
    for d in range(1, n_row):
        pl.semaphore_signal(barrier, inc=1, device_id=((r + d) % n_row, c), device_id_type=MESH)
    for d in range(1, n_col):
        pl.semaphore_signal(barrier, inc=1, device_id=(r, (c + d) % n_col), device_id_type=MESH)
    pl.semaphore_wait(barrier, n_row + n_col - 2)


def part(ref, lead, k, count):
    view = ref if lead is None else ref.at[lead]
    rows = view.shape[0] // count
    return view.at[pl.ds(k * rows, rows)]


def kernel(n_row, n_col, order_1, order_2, ranks, hu, hv, hnear, hsketch, out_u, out_v, *scratch):
    (
        u, v, near, sk, near_t, high, low, p_u, p_v, low_u, low_v, up_u, up_v, above_own, above,
        ex_u, ex_v, ex_w, wide, lower, u1, v1, u1t_own, above1_own, up1t, up1_v, above1,
        low1_u, low1_own, low1_t, send, recv, load,
    ) = scratch
    r, c = lax.axis_index("row"), lax.axis_index("col")
    height, width = u.shape[1:]
    far = 1.0 / (8.0 * height)
    rows_1, rows_2 = above.shape[1], above1.shape[1]
    two = range(2)
    level, side, levels = r // 2, r % 2, n_row // 2
    parity = c % 2
    pieces = []

    def piece(own, ref, root, has, edges, local=False):
        k = len(pieces)
        pieces.append(Piece(own, ref, root, has, edges, send.at[k], recv.at[k], local))
        return pieces[-1]

    other_row, other_col = r + 1 - 2 * side, c + 1 - 2 * parity
    spine = side == parity
    down_on = spine & (level + 1 < levels), (r + 2, c)
    down_over = spine & (level >= 1), (other_row, c)
    down_first = r == 0, (1, c)
    if levels > 1:
        beside = [
            ((r == 0) & (parity == 1), (1, c)),
            ((parity == 0) & (level == 1) & (side == 1), (r - 2, c)),
        ]
    else:
        beside = [down_first]

    def only(cond, edges):
        return [(a & cond, d) for a, d in edges]

    def down(own, ref, when, first):
        return piece(own, ref, (r == 0) & when, (r > 0) & when, only(when, [down_on, down_over] + first))

    def down_1(own, ref, on, when):
        at = side == on
        edges = [
            ((r == 1) & (on == 0), (0, c)),
            (at & (level + 1 < levels), (r + 2, c)),
            (at & (level >= 1), (other_row, c)),
        ]
        return piece(own, ref, (r == 1) & when, ((r > 1) | ((r == 0) & (on == 0))) & when, only(when, edges))

    def across(own, ref, source, when):
        at = parity == source % 2
        edges = [(at, (r, other_col)), (at & (c // 2 + 1 < n_col // 2), (r, c + 2))]
        return piece(own, ref, (c == source) & when, (c != source) & when, only(when, edges), True)

    def pivot(own, ref, k):
        mine = parity == k
        edges = only(mine, [down_first, ((r == 0) & (c + 2 < n_col), (0, c + 2)), down_on, down_over])
        edges.append((mine & (r > 0), (r, other_col)))
        root = (r == 0) & (c == 0)
        if k == 1:
            edges[1] = edges[1][0] | root, (0, jnp.where(root, 1, c + 2))
            edges[0] = edges[0][0] & jnp.logical_not(root), edges[0][1]
        has = jnp.where(mine, jnp.logical_not(root), r > 0)
        return piece(own, ref, root, has, edges)

    quarters, later_rows, always = range(4), r > 1, r >= 0
    pivots = [[pivot(part(a, 0, h, 4), part(b, None, h, 4), k) for h in quarters] for k, a, b in ((0, u, p_u), (1, v, p_v))]
    lows_v = [across(part(v, 0, h, 2), part(low_v, None, h, 2), 0, r > 0) for h in two]
    lows_u = [across(part(u, 0, h, 2), part(low_u, None, h, 2), 0, r > 0) for h in two]
    ups_u = [[down(part(u, t, h, 4), part(up_u, t, h, 4), c > 0 if t == 0 else always, beside if t else [down_first]) for h in quarters] for t in two]
    ups_a = [down(above_own, above, always, [down_first])]
    ups_v = [down(part(v, t, h, 4), part(up_v, t, h, 4), c > 0 if t == 0 else always, beside) for t in two for h in quarters]
    extras = [down_1(part(a, 0, h, 4), part(b, None, h, 4), 0, c == 1) for a, b in ((u, ex_u), (v, ex_v)) for h in quarters]
    extra_w = [down_1(part(wide, 0, h, 4), part(ex_w, None, h, 4), 0, c == 1) for h in quarters]
    chains_u = [
        down_1(part(u1t_own, t, h, 4), up1t.at[t].at[pl.ds(h * (rows_1 // 4), rows_1 // 4)], parity, c > 1 if t == 0 else always)
        for t in two
        for h in quarters
    ]
    chains_a = [down_1(above1_own, above1, parity, always)]
    chains_v = [down_1(part(v1, t, h, 2), part(up1_v, t, h, 2), parity, c > 1 if t == 0 else always) for t in two for h in two]
    lows1_u = [across(part(u1, 0, h, 2), part(low1_u, None, h, 2), 1, later_rows) for h in two]
    lows1_t = [across(part(low1_own, None, h, 2), part(low1_t, None, h, 2), 1, later_rows) for h in two]

    def begin(*groups, only=None):
        for g in groups:
            for x in g:
                x.begin(only)

    def forward(*groups, only=None):
        for g in groups:
            for x in g:
                x.forward(only)

    loads = [(hu, u), (hv, v), (hsketch, sk), (hnear, near)]
    copies = [pltpu.make_async_copy(a, b, load.at[k]) for k, (a, b) in enumerate(loads)]
    for x in copies:
        x.start()
    greet_all(n_row, n_col, r, c)
    for x in copies[:3]:
        x.wait()
    col_id = lax.broadcasted_iota(jnp.int32, (height, width), 1)
    for t in two:
        keep = col_id < ranks[0, 0, t, 0, r]
        u[t] = jnp.where(keep, u[t], 0.0)
        v[t] = jnp.where(keep, v[t], 0.0)
    begin(pivots[1], pivots[0], lows_v, lows_u, extras)
    sketch_t = [split(sk[k].T[:rows]) for k, rows in ((0, rows_1), (1, rows_2))]

    def here_of(v, k):
        both = stacked(sketch_t[k], split(jnp.concatenate([v[0], v[1]], axis=1)))
        return both[:, :width], both[:, width:]

    @pl.when(r == 0)
    def _():
        for t in two:
            begin(ups_u[t], only=parity != t)
        forward(pivots[0], pivots[1])
        for t in two:
            begin(ups_u[t], only=parity == t)
        a, b = here_of(v, 0)
        above_own[0] = a
        above_own[1] = b
        begin(ups_a, ups_v)
        copies[3].wait()
        for t in two:
            stays = (c > 0) | (t > 0)
            out_u[t] = jnp.where(stays, u[t], 0.0)
            out_v[t] = jnp.where(stays, v[t], 0.0)
        forward(extras, extra_w, chains_u, chains_a, chains_v)

    @pl.when((r > 0) & (c == 0))
    def _():
        up_u[0] = jnp.zeros((height, width), F32)
        up_v[0] = jnp.zeros((height, width), F32)

    @pl.when(r > 0)
    def _():
        for t in two:
            up1t[t, rows_1:] = jnp.zeros((width - rows_1, height), F32)

        @pl.when(c < 2)
        def _():
            up1t[0, :rows_1] = jnp.zeros((rows_1, height), F32)
            up1_v[0] = jnp.zeros((height, width), F32)

        copies[3].wait()
        near_t[0] = near[0].T

        @pl.when((c == 1) & later_rows)
        def _():
            near_t[1] = near[1].T

        scale = diagonal_inverse(near[0])
        here = here_of(v, 0)
        last = level + 1 == levels
        relays = later_rows & jnp.logical_not(last) & (spine | ((level == 1) & (parity == 0)))
        ends = later_rows & jnp.logical_not(relays)
        middle = ((r == 1) & (parity == 1)) | (last & spine)
        passes = relays | ((r == 1) & (parity == 1))
        leads = lambda cond: [forward(ups_u[t], only=passes & (parity != t) & cond) for t in two]
        forward(extras, only=later_rows & (side == 0))
        leads(c >= 2)
        for k in two:
            forward(pivots[k], only=parity == k)
        leads(c < 2)
        for t in two:
            forward(ups_u[t], only=relays & (parity == t))
        forward(ups_a, only=relays)
        early = relays & (level == 1) & (parity == 0)
        forward(ups_v, only=early)
        forward(lows_v, lows_u)
        for k in two:
            forward(pivots[k], only=parity != k)
        pivot_t = near_t[0] + far * deep(split(p_v[...]), split(p_u[...]), 1)
        high[...], low[...] = split(pivot_t)
        def hook(k):
            for t in two:
                if k < 4:
                    forward(ups_u[t][k : k + 1], only=ends & (parity != t))
                else:
                    forward(ups_u[t][k - 4 : k - 3], only=(ends | ((r == 1) & (parity == 1))) & (parity == t))

        hooks = {k: functools.partial(hook, k) for k in range(7)}
        lower[...] = apply_inverse(high, low, scale, low_v[...], hooks)
        hook(7)
        forward(ups_u[1], ups_u[0], only=(r == 1) & (parity == 0))
        forward(extras, only=later_rows & (side == 1))
        forward(extra_w, only=later_rows & (side == 0))
        forward(ups_a, only=jnp.logical_not(relays))
        forward(ups_v, only=relays & jnp.logical_not(early))
        core = far * stacked(
            split(lower[...].T), split(jnp.concatenate([up_u[0], up_u[1]], axis=1))
        )
        lane = lax.broadcasted_iota(jnp.int32, core.shape, 1)
        live = (lane < ranks[0, 0, 0, 0, 0]) | ((lane >= width) & (lane < width + ranks[0, 0, 1, 0, 0]))
        core = jnp.where(live, core, 0.0)
        both = deep(split(low_u[...]), split(core))
        wide[0] = both[:, :width]
        wide[1] = both[:, width:]
        begin(extra_w)
        rank_1 = [ranks[1, 0, t, 0, r] for t in two]
        bases = [basis_of(here[t], above[t], u[t], wide[t], rank_1[t]) for t in two]
        bases = orthonormal(bases, rank_1, order_1, width)
        forward(ups_v, only=middle)
        forward(extra_w, only=later_rows & (side == 1))
        orthos = orthonormal(bases, rank_1, order_1, width)
        root_order = math.sqrt(height)
        tile_col = [t * n_col + c for t in two]
        chosen = [(tile_col[t] > 0) & jnp.logical_not((r == 1) & (tile_col[t] == 1)) for t in two]
        for t in two:
            u1t_own[t] = orthos[t] * root_order
        begin(chains_u)
        for t in two:
            u1[t] = jnp.where(chosen[t], pad_rows(orthos[t] * root_order, width).T, u[t])
        begin(lows1_u)
        forward(ups_v, only=jnp.logical_not(relays | middle))
        for t in two:
            right = new_right(backward(orthos[t], u[t], wide[t]), v[t], up_v[t]) * (1.0 / root_order)
            v1[t] = jnp.where(chosen[t], right, jnp.where(tile_col[t] == 0, lower[...], v[t]))
        here = here_of(v1, 1)
        above1_own[0] = here[0]
        above1_own[1] = here[1]
        begin(chains_a, chains_v)

        @pl.when(r == 1)
        def _():
            out_u[...] = u1[...]
            out_v[...] = v1[...]

        @pl.when(later_rows)
        def _():
            @pl.when(c == 1)
            def _():
                left = jnp.concatenate([ex_v[...], up_v[0]], axis=1)
                right = jnp.concatenate([ex_u[...], -ex_w[...]], axis=1)
                lh, ll = split(left)
                rh, rl = split(right)
                pivot_t = near_t[1] + far * (mm(lh, rh, 1) + (mm(lh, rl, 1) + mm(ll, rh, 1)))
                high[...], low[...] = split(pivot_t)
                lower[...] = apply_inverse(high, low, diagonal_inverse(near[1]), v1[0], {})
                low1_own[...] = lower[...].T[:rows_1]

            begin(lows1_t)
            forward(chains_u, chains_a)
            forward(chains_v, only=spine)
            forward(lows1_u, lows1_t)
            core = far * stacked(split(low1_t[...]), split(up1t[...].reshape(2 * width, height)), 1)
            both = deep(split(low1_u[...]), split(pad_rows(core, width)))
            wide[0] = both[:, :width]
            wide[1] = both[:, width:]
            rank_2 = [ranks[2, 0, t, 0, r] for t in two]
            bases = [basis_of(here[t], above1[t], u1[t], wide[t], rank_2[t]) for t in two]
            bases = orthonormal(bases, rank_2, order_2, width)
            orthos = orthonormal(bases, rank_2, order_2, width)
            forward(chains_v, only=jnp.logical_not(spine))
            for t in two:
                live = tile_col[t] > 1
                right = new_right(backward(orthos[t], u1[t], wide[t]), v1[t], up1_v[t]) * (1.0 / root_order)
                out_u[t] = jnp.where(live, pad_rows(orthos[t] * root_order, width).T, u1[t])
                out_v[t] = jnp.where(live, right, jnp.where(tile_col[t] == 1, lower[...], v1[t]))

    for x in pieces:
        x.finish()


def body(n_row, n_col, factor_u, factor_v, near_field, sketch, tile_ranks):
    tiles, height, width = factor_u.shape[2], factor_u.shape[4], factor_u.shape[5]
    u = factor_u.reshape(tiles, height, width)
    v = factor_v.reshape(tiles, height, width)
    ranks = jnp.transpose(tile_ranks, (0, 1, 3, 4, 2))
    pair, one = (tiles, height, width), (height, width)
    order_1 = width - max(1, width // 4)
    order_2 = order_1 - max(1, order_1 // 4)
    rows_1, rows_2 = -(-order_1 // 16) * 16, -(-order_2 // 16) * 16
    square = (height, height)
    f32 = lambda *shape: pltpu.VMEM(shape, F32)
    buffers = [f32(*s) for s in (pair, pair, (2,) + square, (2,) + one, (2,) + square)]
    buffers += [pltpu.VMEM(square, BF16)] * 2
    buffers += [f32(*s) for s in (one, one, one, one, pair, pair, (2, rows_1, width), (2, rows_1, width))]
    buffers += [f32(*s) for s in (one, one, one, pair, one, pair, pair, (2, rows_1, height), (2, rows_2, width))]
    buffers += [f32(*s) for s in ((2, width, height), pair, (2, rows_2, width), one, (rows_1, height), (rows_1, height))]
    pieces = 58
    any_spec = pl.BlockSpec(memory_space=pl.ANY)
    out_u, out_v = pl.pallas_call(
        functools.partial(kernel, n_row, n_col, order_1, order_2),
        out_shape=[jax.ShapeDtypeStruct(pair, F32)] * 2,
        in_specs=[pl.BlockSpec(memory_space=pltpu.SMEM)] + [any_spec] * 4,
        out_specs=[pl.BlockSpec(memory_space=pltpu.VMEM)] * 2,
        scratch_shapes=buffers
        + [
            pltpu.SemaphoreType.DMA((pieces, EDGES)),
            pltpu.SemaphoreType.DMA((pieces,)),
            pltpu.SemaphoreType.DMA((4,)),
        ],
        compiler_params=pltpu.CompilerParams(
            collective_id=0, has_side_effects=True, vmem_limit_bytes=60 * 1024 * 1024
        ),
    )(ranks, u, v, near_field, sketch)
    tile_col = jnp.arange(tiles, dtype=jnp.int32) * n_col + lax.axis_index("col")
    stays = jnp.logical_not((lax.axis_index("row") == 1) & (tile_col == 1))[:, None, None]
    out_u, out_v = jnp.where(stays, out_u, 0.0), jnp.where(stays, out_v, 0.0)
    shape_out = (1, 1, tiles, 1, height, width)
    return (out_u.reshape(shape_out), out_v.reshape(shape_out))


def solution(mesh):
    tile_spec = P(None, "row", None, "col", None, None)
    return jax.shard_map(
        functools.partial(body, mesh.shape["row"], mesh.shape["col"]),
        mesh=mesh,
        in_specs=(tile_spec, tile_spec, P(), P(), P(None, None, None, None, "col")),
        out_specs=(tile_spec, tile_spec),
        check_vma=False,
    )
```

```python
import functools
import math

import jax
import jax.numpy as jnp
from jax import lax
from jax.experimental import pallas as pl
from jax.experimental.pallas import tpu as pltpu
from jax.sharding import PartitionSpec as P

NS_STEPS = 3
BLOCK = 16
EDGES = 5
F32 = jnp.float32
BF16 = jnp.bfloat16
MESH = pl.DeviceIdType.MESH


def split(x):
    high = x.astype(BF16)
    return high, (x - high.astype(F32)).astype(BF16)


def mm(a, b, contract_b=0):
    return lax.dot_general(a, b, (((1,), (contract_b,)), ((), ())), preferred_element_type=F32)


def stacked(a, b, contract_b=0):
    ah, al = a
    bh, bl = b
    n = ah.shape[0]
    both = mm(jnp.concatenate([ah, al], axis=0), bh, contract_b)
    return both[:n] + both[n:] + mm(ah, bl, contract_b)


def deep(a, b, contract_b=0):
    ah, al = a
    bh, bl = b
    axis = contract_b
    return mm(jnp.concatenate([ah, al], axis=1), jnp.concatenate([bh, bh], axis=axis), contract_b) + mm(
        ah, bl, contract_b
    )


def pad_rows(x, n):
    if x.shape[0] == n:
        return x
    return jnp.concatenate([x, jnp.zeros((n - x.shape[0], x.shape[1]), x.dtype)], axis=0)


def apply_inverse(high, low, scale, w, hooks):
    n = w.shape[1]
    x = scale * w
    for step in range(2**NS_STEPS - 1):
        xh, xl = split(x)
        both = mm(high[...], jnp.concatenate([xh, xl], axis=1))
        x = x + scale * (w - (both[:, :n] + both[:, n:] + mm(low[...], xh)))
        if step in hooks:
            hooks[step]()
    return x


def diagonal_inverse(near):
    n = near.shape[0]
    eye = lax.broadcasted_iota(jnp.int32, (n, n), 0) == lax.broadcasted_iota(jnp.int32, (n, n), 1)
    return 1.0 / jnp.sum(jnp.where(eye, near, 0.0), axis=1, keepdims=True)


def spread(x, j):
    return jnp.broadcast_to(x[:, j : j + 1], x.shape)


def whiten(grams, rights, order):
    count, width = len(grams), grams[0].shape[1]
    total = grams[0].shape[0]
    rest = [jnp.concatenate([g, x], axis=1) for g, x in zip(grams, rights)]
    done = [[] for _ in grams]
    start = 0
    while start < order:
        size = min(BLOCK, order - start)
        end = start + size
        tiles = size // 8
        row_id = lax.broadcasted_iota(jnp.int32, (1, 8, width), 1)
        column = lambda x, h, j: jnp.broadcast_to(x[8 * h : 8 * h + 8, start + j : start + j + 1], (8, width))
        cols = [
            [None if h < j // 8 else jnp.stack([column(x, h, j) for x in rest]) for h in range(tiles)]
            for j in range(size)
        ]
        rows = [jnp.stack([x[8 * h : 8 * h + 8] for x in rest]) for h in range(tiles)]
        lanes = rows[0].shape[2] // width
        along = lambda m: jnp.concatenate([m] * lanes, axis=2)
        scale = [jnp.ones((count, 8, width), F32) for _ in range(tiles)]
        for k in range(size):
            hk, rk = k // 8, k % 8
            lead = cols[k]
            inv = lax.rsqrt(spread(lead[hk], rk))
            inv2 = inv * inv
            masked = list(lead)
            masked[hk] = jnp.where(row_id > rk, lead[hk], 0.0)
            m = [None if x is None else x * inv2 for x in masked]
            for j in range(k + 1, size):
                hj, rj = j // 8, j % 8
                x = spread(lead[hj], rj)
                for h in range(hj, tiles):
                    step = (masked[h] * x) * inv2 if j == k + 1 else m[h] * x
                    cols[j][h] = cols[j][h] - step
            top = rows[hk][:, rk : rk + 1]
            for h in range(hk, tiles):
                rows[h] = rows[h] - along(m[h]) * top
            scale[hk] = jnp.where(row_id == rk, inv, scale[hk])
        rows = [x * along(s) for x, s in zip(rows, scale)]
        block = jnp.concatenate(rows, axis=1) if tiles > 1 else rows[0]
        for t in range(count):
            done[t].append(block[t][:, width:])
        if end < order:
            new = []
            for t in range(count):
                high = block[t].astype(BF16).astype(F32)
                low = block[t] - high
                left = [high[:, :width], low[:, :width], high[:, :width]]
                left = jnp.concatenate(left, axis=0).T[end:order].astype(BF16)
                right = jnp.concatenate([high, high, low], axis=0).astype(BF16)
                new.append(rest[t][size : order - start] - mm(left, right))
            rest = new
        start = end
    return [pad_rows(jnp.concatenate(d, axis=0), total) for d in done]


def orthonormal(bases, ranks, order, width):
    count = bases[0].shape[0]
    row = lax.broadcasted_iota(jnp.int32, (count, width), 0)
    col = lax.broadcasted_iota(jnp.int32, (count, width), 1)
    grams = []
    for basis, rank in zip(bases, ranks):
        high, low = split(basis)
        gram = stacked((high, low), (pad_rows(high, width), pad_rows(low, width)), 1)
        grams.append(gram + jnp.where((row == col) & (col >= rank), 1.0, 0.0))
    return whiten(grams, bases, order)


def basis_of(here, above, u, wide, rank):
    rows = here.shape[0]
    keep = lax.broadcasted_iota(jnp.int32, (rows, 2 * here.shape[1]), 0) < rank
    both = jnp.where(keep, jnp.concatenate([here, -above], axis=1), 0.0)
    return stacked(split(both), split(jnp.concatenate([u, wide], axis=1)), 1)


def backward(ortho, u, wide):
    back = stacked(split(ortho), split(jnp.concatenate([u, wide], axis=1)))
    width = u.shape[1]
    return jnp.concatenate([back[:, :width], -back[:, width:]], axis=1)


def new_right(back, v, up):
    width = v.shape[1]
    bh, bl = split(back)
    bh, bl = pad_rows(bh, width), pad_rows(bl, width)
    vh, vl = split(jnp.concatenate([v, up], axis=1))
    both = mm(vh, jnp.concatenate([bh, bl], axis=0), 1)
    return both[:, :width] + both[:, width:] + mm(vl, bh, 1)


class Piece:
    def __init__(self, own, ref, root, has, edges, send, recv, local=False):
        self.own, self.ref, self.root, self.has, self.edges = own, ref, root, has, edges
        self.send, self.recv, self.local = send, recv, local

    def copy(self, k, src):
        return pltpu.make_async_remote_copy(
            src_ref=src,
            dst_ref=self.ref,
            send_sem=self.send.at[k],
            recv_sem=self.recv,
            device_id=self.edges[k][1],
            device_id_type=MESH,
        )

    def send_all(self, src):
        for k, (cond, _) in enumerate(self.edges):
            @pl.when(cond)
            def _(k=k):
                self.copy(k, src).start()

    def begin(self, only=None):
        @pl.when(self.root if only is None else self.root & only)
        def _():
            self.send_all(self.own)
            if self.local:
                pltpu.make_async_copy(self.own, self.ref, self.recv).start()

    def forward(self, only=None):
        both = lambda cond: cond if only is None else cond & only
        if self.local:
            @pl.when(both(self.root))
            def _():
                pltpu.make_async_copy(self.ref, self.ref, self.recv).wait()

        @pl.when(both(self.has))
        def _():
            pltpu.make_async_copy(self.ref, self.ref, self.recv).wait()
            self.send_all(self.ref)

    def finish(self):
        @pl.when(self.root | self.has)
        def _():
            for k, (cond, _) in enumerate(self.edges):
                @pl.when(cond)
                def _(k=k):
                    self.copy(k, self.ref).wait_send()


def greet_all(n_row, n_col, r, c):
    barrier = pltpu.get_barrier_semaphore()
    for d in range(1, n_row):
        pl.semaphore_signal(barrier, inc=1, device_id=((r + d) % n_row, c), device_id_type=MESH)
    for d in range(1, n_col):
        pl.semaphore_signal(barrier, inc=1, device_id=(r, (c + d) % n_col), device_id_type=MESH)
    pl.semaphore_wait(barrier, n_row + n_col - 2)


def part(ref, lead, k, count):
    view = ref if lead is None else ref.at[lead]
    rows = view.shape[0] // count
    return view.at[pl.ds(k * rows, rows)]


def kernel(n_row, n_col, order_1, order_2, ranks, hu, hv, hnear, hsketch, out_u, out_v, *scratch):
    (
        u, v, near, sk, near_t, high, low, p_u, p_v, low_u, low_v, up_u, up_v, above_own, above,
        ex_u, ex_v, ex_w, wide, lower, u1, v1, u1t_own, above1_own, up1t, up1_v, above1,
        low1_u, low1_own, low1_t, send, recv, load,
    ) = scratch
    r, c = lax.axis_index("row"), lax.axis_index("col")
    height, width = u.shape[1:]
    far = 1.0 / (8.0 * height)
    rows_1, rows_2 = above.shape[1], above1.shape[1]
    two = range(2)
    level, side, levels = r // 2, r % 2, n_row // 2
    parity = c % 2
    pieces = []

    def piece(own, ref, root, has, edges, local=False):
        k = len(pieces)
        pieces.append(Piece(own, ref, root, has, edges, send.at[k], recv.at[k], local))
        return pieces[-1]

    other_row, other_col = r + 1 - 2 * side, c + 1 - 2 * parity
    spine = side == parity
    down_on = spine & (level + 1 < levels), (r + 2, c)
    down_over = spine & (level >= 1), (other_row, c)
    down_first = r == 0, (1, c)
    if levels > 1:
        beside = [
            ((r == 0) & (parity == 1), (1, c)),
            ((parity == 0) & (level == 1) & (side == 1), (r - 2, c)),
        ]
    else:
        beside = [down_first]

    def only(cond, edges):
        return [(a & cond, d) for a, d in edges]

    def down(own, ref, when, first):
        return piece(own, ref, (r == 0) & when, (r > 0) & when, only(when, [down_on, down_over] + first))

    def down_1(own, ref, on, when):
        at = side == on
        edges = [
            ((r == 1) & (on == 0), (0, c)),
            (at & (level + 1 < levels), (r + 2, c)),
            (at & (level >= 1), (other_row, c)),
        ]
        return piece(own, ref, (r == 1) & when, ((r > 1) | ((r == 0) & (on == 0))) & when, only(when, edges))

    def across(own, ref, source, when):
        at = parity == source % 2
        edges = [(at, (r, other_col)), (at & (c // 2 + 1 < n_col // 2), (r, c + 2))]
        return piece(own, ref, (c == source) & when, (c != source) & when, only(when, edges), True)

    def pivot(own, ref, k):
        mine = parity == k
        edges = only(mine, [down_first, ((r == 0) & (c + 2 < n_col), (0, c + 2)), down_on, down_over])
        edges.append((mine & (r > 0), (r, other_col)))
        root = (r == 0) & (c == 0)
        if k == 1:
            edges[1] = edges[1][0] | root, (0, jnp.where(root, 1, c + 2))
            edges[0] = edges[0][0] & jnp.logical_not(root), edges[0][1]
        has = jnp.where(mine, jnp.logical_not(root), r > 0)
        return piece(own, ref, root, has, edges)

    quarters, later_rows, always = range(4), r > 1, r >= 0
    pivots = [[pivot(part(a, 0, h, 4), part(b, None, h, 4), k) for h in quarters] for k, a, b in ((0, u, p_u), (1, v, p_v))]
    lows_v = [across(part(v, 0, h, 2), part(low_v, None, h, 2), 0, r > 0) for h in two]
    lows_u = [across(part(u, 0, h, 2), part(low_u, None, h, 2), 0, r > 0) for h in two]
    ups_u = [[down(part(u, t, h, 4), part(up_u, t, h, 4), c > 0 if t == 0 else always, beside if t else [down_first]) for h in quarters] for t in two]
    ups_a = [down(above_own, above, always, [down_first])]
    ups_v = [down(part(v, t, h, 4), part(up_v, t, h, 4), c > 0 if t == 0 else always, beside) for t in two for h in quarters]
    extras = [down_1(part(a, 0, h, 4), part(b, None, h, 4), 0, c == 1) for a, b in ((u, ex_u), (v, ex_v)) for h in quarters]
    extra_w = [down_1(part(wide, 0, h, 4), part(ex_w, None, h, 4), 0, c == 1) for h in quarters]
    chains_u = [
        down_1(part(u1t_own, t, h, 4), up1t.at[t].at[pl.ds(h * (rows_1 // 4), rows_1 // 4)], parity, c > 1 if t == 0 else always)
        for t in two
        for h in quarters
    ]
    chains_a = [down_1(above1_own, above1, parity, always)]
    chains_v = [down_1(part(v1, t, h, 2), part(up1_v, t, h, 2), parity, c > 1 if t == 0 else always) for t in two for h in two]
    lows1_u = [across(part(u1, 0, h, 2), part(low1_u, None, h, 2), 1, later_rows) for h in two]
    lows1_t = [across(part(low1_own, None, h, 2), part(low1_t, None, h, 2), 1, later_rows) for h in two]

    def begin(*groups, only=None):
        for g in groups:
            for x in g:
                x.begin(only)

    def forward(*groups, only=None):
        for g in groups:
            for x in g:
                x.forward(only)

    loads = [(hu, u), (hv, v), (hsketch, sk), (hnear, near)]
    copies = [pltpu.make_async_copy(a, b, load.at[k]) for k, (a, b) in enumerate(loads)]
    for x in copies:
        x.start()
    greet_all(n_row, n_col, r, c)
    for x in copies[:3]:
        x.wait()
    col_id = lax.broadcasted_iota(jnp.int32, (height, width), 1)
    for t in two:
        keep = col_id < ranks[0, 0, t, 0, r]
        u[t] = jnp.where(keep, u[t], 0.0)
        v[t] = jnp.where(keep, v[t], 0.0)
    begin(pivots[1], pivots[0], lows_v, lows_u, extras)
    sketch_t = [split(sk[k].T[:rows]) for k, rows in ((0, rows_1), (1, rows_2))]

    def here_of(v, k):
        both = stacked(sketch_t[k], split(jnp.concatenate([v[0], v[1]], axis=1)))
        return both[:, :width], both[:, width:]

    @pl.when(r == 0)
    def _():
        for t in two:
            begin(ups_u[t], only=parity != t)
        forward(pivots[0], pivots[1])
        for t in two:
            begin(ups_u[t], only=parity == t)
        a, b = here_of(v, 0)
        above_own[0] = a
        above_own[1] = b
        begin(ups_a, ups_v)
        copies[3].wait()
        for t in two:
            stays = (c > 0) | (t > 0)
            out_u[t] = jnp.where(stays, u[t], 0.0)
            out_v[t] = jnp.where(stays, v[t], 0.0)
        forward(extras, extra_w, chains_u, chains_a, chains_v)

    @pl.when((r > 0) & (c == 0))
    def _():
        up_u[0] = jnp.zeros((height, width), F32)
        up_v[0] = jnp.zeros((height, width), F32)

    @pl.when(r > 0)
    def _():
        for t in two:
            up1t[t, rows_1:] = jnp.zeros((width - rows_1, height), F32)

        @pl.when(c < 2)
        def _():
            up1t[0, :rows_1] = jnp.zeros((rows_1, height), F32)
            up1_v[0] = jnp.zeros((height, width), F32)

        copies[3].wait()
        near_t[0] = near[0].T

        @pl.when((c == 1) & later_rows)
        def _():
            near_t[1] = near[1].T

        scale = diagonal_inverse(near[0])
        here = here_of(v, 0)
        last = level + 1 == levels
        relays = later_rows & jnp.logical_not(last) & (spine | ((level == 1) & (parity == 0)))
        ends = later_rows & jnp.logical_not(relays)
        odd = parity == 1
        prompt = relays & (parity == 0)
        middle = (odd & ((r == 1) | relays)) | (last & spine & (parity == 0))
        late = jnp.logical_not(prompt | middle)
        first_on = spine & jnp.logical_not(last) & ((level == 1) | (c != 1))
        soon = first_on & odd & (level == 1)
        passes = relays | ((r == 1) & (parity == 1))
        leads = lambda cond: [forward(ups_u[t], only=passes & (parity != t) & cond) for t in two]
        forward(extras, only=later_rows & (side == 0))
        leads(c >= 2)
        forward(lows_v, only=parity == 0)
        for k in two:
            forward(pivots[k], only=parity == k)
        leads(c < 2)
        forward(lows_u, only=parity == 0)
        forward(ups_u[0], ups_a, only=relays & (parity == 0))
        early = relays & (level == 1) & (parity == 0)
        forward(ups_v, only=early)
        forward(lows_v, only=odd)
        for k in two:
            forward(pivots[k], only=parity != k)
        pivot_t = near_t[0] + far * deep(split(p_v[...]), split(p_u[...]), 1)
        high[...], low[...] = split(pivot_t)
        def hook(k):
            for t in two:
                if k < 4:
                    forward(ups_u[t][k : k + 1], only=ends & (parity != t))
                else:
                    forward(ups_u[t][k - 4 : k - 3], only=(ends | odd) & (parity == t))

        hooks = {k: functools.partial(hook, k) for k in range(7)}
        lower[...] = apply_inverse(high, low, scale, low_v[...], hooks)
        hook(7)
        forward(ups_u[1], ups_u[0], only=(r == 1) & (parity == 0))
        forward(extras, only=later_rows & (side == 1))
        forward(extra_w, only=later_rows & (side == 0))
        forward(lows_u, only=odd)
        forward(ups_a, only=odd | jnp.logical_not(relays))
        forward(ups_v, only=prompt & jnp.logical_not(early))
        core = far * stacked(
            split(lower[...].T), split(jnp.concatenate([up_u[0], up_u[1]], axis=1))
        )
        lane = lax.broadcasted_iota(jnp.int32, core.shape, 1)
        live = (lane < ranks[0, 0, 0, 0, 0]) | ((lane >= width) & (lane < width + ranks[0, 0, 1, 0, 0]))
        core = jnp.where(live, core, 0.0)
        both = deep(split(low_u[...]), split(core))
        wide[0] = both[:, :width]
        wide[1] = both[:, width:]
        begin(extra_w)
        rank_1 = [ranks[1, 0, t, 0, r] for t in two]
        bases = [basis_of(here[t], above[t], u[t], wide[t], rank_1[t]) for t in two]
        bases = orthonormal(bases, rank_1, order_1, width)
        forward(ups_v, only=middle)
        forward(chains_u, only=later_rows & soon)
        forward(extra_w, only=later_rows & (side == 1))
        orthos = orthonormal(bases, rank_1, order_1, width)
        root_order = math.sqrt(height)
        tile_col = [t * n_col + c for t in two]
        chosen = [(tile_col[t] > 0) & jnp.logical_not((r == 1) & (tile_col[t] == 1)) for t in two]
        for t in two:
            u1t_own[t] = orthos[t] * root_order
        begin(chains_u)
        for t in two:
            u1[t] = jnp.where(chosen[t], pad_rows(orthos[t] * root_order, width).T, u[t])
        begin(lows1_u)
        forward(chains_u, only=later_rows & first_on & jnp.logical_not(soon))

        def right_of(t):
            right = new_right(backward(orthos[t], u[t], wide[t]), v[t], up_v[t]) * (1.0 / root_order)
            return jnp.where(chosen[t], right, jnp.where(tile_col[t] == 0, lower[...], v[t]))

        forward(ups_v[:4], only=late)
        v1[0] = right_of(0)

        @pl.when((c == 1) & later_rows)
        def _():
            left = jnp.concatenate([ex_v[...], up_v[0]], axis=1)
            right = jnp.concatenate([ex_u[...], -ex_w[...]], axis=1)
            lh, ll = split(left)
            rh, rl = split(right)
            pivot_t = near_t[1] + far * (mm(lh, rh, 1) + (mm(lh, rl, 1) + mm(ll, rh, 1)))
            high[...], low[...] = split(pivot_t)
            lower[...] = apply_inverse(high, low, diagonal_inverse(near[1]), v1[0], {})
            low1_own[...] = lower[...].T[:rows_1]

        begin(lows1_t)
        forward(lows1_u, only=later_rows & odd)
        forward(ups_v[4:], only=late)
        v1[1] = right_of(1)
        here = here_of(v1, 1)
        above1_own[0] = here[0]
        above1_own[1] = here[1]
        begin(chains_a, chains_v)

        @pl.when(r == 1)
        def _():
            out_u[...] = u1[...]
            out_v[...] = v1[...]

        @pl.when(later_rows)
        def _():
            forward(chains_u, only=jnp.logical_not(first_on))
            forward(chains_a)
            forward(lows1_t, only=odd)
            forward(chains_v, only=spine & jnp.logical_not(last & odd))
            forward(lows1_u, lows1_t, only=parity == 0)
            core = far * stacked(split(low1_t[...]), split(up1t[...].reshape(2 * width, height)), 1)
            both = deep(split(low1_u[...]), split(pad_rows(core, width)))
            wide[0] = both[:, :width]
            wide[1] = both[:, width:]
            rank_2 = [ranks[2, 0, t, 0, r] for t in two]
            bases = [basis_of(here[t], above1[t], u1[t], wide[t], rank_2[t]) for t in two]
            bases = orthonormal(bases, rank_2, order_2, width)
            forward(chains_v, only=spine & last & odd)
            orthos = orthonormal(bases, rank_2, order_2, width)
            forward(chains_v, only=jnp.logical_not(spine))
            for t in two:
                live = tile_col[t] > 1
                right = new_right(backward(orthos[t], u1[t], wide[t]), v1[t], up1_v[t]) * (1.0 / root_order)
                out_u[t] = jnp.where(live, pad_rows(orthos[t] * root_order, width).T, u1[t])
                out_v[t] = jnp.where(live, right, jnp.where(tile_col[t] == 1, lower[...], v1[t]))

    for x in pieces:
        x.finish()


def body(n_row, n_col, factor_u, factor_v, near_field, sketch, tile_ranks):
    tiles, height, width = factor_u.shape[2], factor_u.shape[4], factor_u.shape[5]
    u = factor_u.reshape(tiles, height, width)
    v = factor_v.reshape(tiles, height, width)
    ranks = jnp.transpose(tile_ranks, (0, 1, 3, 4, 2))
    pair, one = (tiles, height, width), (height, width)
    order_1 = width - max(1, width // 4)
    order_2 = order_1 - max(1, order_1 // 4)
    rows_1, rows_2 = -(-order_1 // 16) * 16, -(-order_2 // 16) * 16
    square = (height, height)
    f32 = lambda *shape: pltpu.VMEM(shape, F32)
    buffers = [f32(*s) for s in (pair, pair, (2,) + square, (2,) + one, (2,) + square)]
    buffers += [pltpu.VMEM(square, BF16)] * 2
    buffers += [f32(*s) for s in (one, one, one, one, pair, pair, (2, rows_1, width), (2, rows_1, width))]
    buffers += [f32(*s) for s in (one, one, one, pair, one, pair, pair, (2, rows_1, height), (2, rows_2, width))]
    buffers += [f32(*s) for s in ((2, width, height), pair, (2, rows_2, width), one, (rows_1, height), (rows_1, height))]
    pieces = 58
    any_spec = pl.BlockSpec(memory_space=pl.ANY)
    out_u, out_v = pl.pallas_call(
        functools.partial(kernel, n_row, n_col, order_1, order_2),
        out_shape=[jax.ShapeDtypeStruct(pair, F32)] * 2,
        in_specs=[pl.BlockSpec(memory_space=pltpu.SMEM)] + [any_spec] * 4,
        out_specs=[pl.BlockSpec(memory_space=pltpu.VMEM)] * 2,
        scratch_shapes=buffers
        + [
            pltpu.SemaphoreType.DMA((pieces, EDGES)),
            pltpu.SemaphoreType.DMA((pieces,)),
            pltpu.SemaphoreType.DMA((4,)),
        ],
        compiler_params=pltpu.CompilerParams(
            collective_id=0, has_side_effects=True, vmem_limit_bytes=60 * 1024 * 1024
        ),
    )(ranks, u, v, near_field, sketch)
    tile_col = jnp.arange(tiles, dtype=jnp.int32) * n_col + lax.axis_index("col")
    stays = jnp.logical_not((lax.axis_index("row") == 1) & (tile_col == 1))[:, None, None]
    out_u, out_v = jnp.where(stays, out_u, 0.0), jnp.where(stays, out_v, 0.0)
    shape_out = (1, 1, tiles, 1, height, width)
    return (out_u.reshape(shape_out), out_v.reshape(shape_out))


def solution(mesh):
    tile_spec = P(None, "row", None, "col", None, None)
    return jax.shard_map(
        functools.partial(body, mesh.shape["row"], mesh.shape["col"]),
        mesh=mesh,
        in_specs=(tile_spec, tile_spec, P(), P(), P(None, None, None, None, "col")),
        out_specs=(tile_spec, tile_spec),
        check_vma=False,
    )
```

```python
import functools
import math

import jax
import jax.numpy as jnp
from jax import lax
from jax.experimental import pallas as pl
from jax.experimental.pallas import tpu as pltpu
from jax.sharding import PartitionSpec as P

NS_STEPS = 3
BLOCK = 16
EDGES = 5
F32 = jnp.float32
BF16 = jnp.bfloat16
MESH = pl.DeviceIdType.MESH


def split(x):
    high = x.astype(BF16)
    return high, (x - high.astype(F32)).astype(BF16)


def mm(a, b, contract_b=0):
    return lax.dot_general(a, b, (((1,), (contract_b,)), ((), ())), preferred_element_type=F32)


def stacked(a, b, contract_b=0):
    ah, al = a
    bh, bl = b
    n = ah.shape[0]
    both = mm(jnp.concatenate([ah, al], axis=0), bh, contract_b)
    return both[:n] + both[n:] + mm(ah, bl, contract_b)


def deep(a, b, contract_b=0):
    ah, al = a
    bh, bl = b
    axis = contract_b
    return mm(jnp.concatenate([ah, al], axis=1), jnp.concatenate([bh, bh], axis=axis), contract_b) + mm(
        ah, bl, contract_b
    )


def pad_rows(x, n):
    if x.shape[0] == n:
        return x
    return jnp.concatenate([x, jnp.zeros((n - x.shape[0], x.shape[1]), x.dtype)], axis=0)


def apply_inverse(high, low, scale, w, hooks):
    n = w.shape[1]
    x = scale * w
    for step in range(2**NS_STEPS - 1):
        xh, xl = split(x)
        both = mm(high[...], jnp.concatenate([xh, xl], axis=1))
        x = x + scale * (w - (both[:, :n] + both[:, n:] + mm(low[...], xh)))
        if step in hooks:
            hooks[step]()
    return x


def diagonal_inverse(near):
    n = near.shape[0]
    eye = lax.broadcasted_iota(jnp.int32, (n, n), 0) == lax.broadcasted_iota(jnp.int32, (n, n), 1)
    return 1.0 / jnp.sum(jnp.where(eye, near, 0.0), axis=1, keepdims=True)


def spread(x, j):
    return jnp.broadcast_to(x[:, j : j + 1], x.shape)


def whiten(grams, rights, order):
    count, width = len(grams), grams[0].shape[1]
    total = grams[0].shape[0]
    rest = [jnp.concatenate([g, x], axis=1) for g, x in zip(grams, rights)]
    done = [[] for _ in grams]
    start = 0
    while start < order:
        size = min(BLOCK, order - start)
        end = start + size
        tiles = size // 8
        row_id = lax.broadcasted_iota(jnp.int32, (1, 8, width), 1)
        column = lambda x, h, j: jnp.broadcast_to(x[8 * h : 8 * h + 8, start + j : start + j + 1], (8, width))
        cols = [
            [None if h < j // 8 else jnp.stack([column(x, h, j) for x in rest]) for h in range(tiles)]
            for j in range(size)
        ]
        rows = [jnp.stack([x[8 * h : 8 * h + 8] for x in rest]) for h in range(tiles)]
        lanes = rows[0].shape[2] // width
        along = lambda m: jnp.concatenate([m] * lanes, axis=2)
        scale = [jnp.ones((count, 8, width), F32) for _ in range(tiles)]
        for k in range(size):
            hk, rk = k // 8, k % 8
            lead = cols[k]
            inv = lax.rsqrt(spread(lead[hk], rk))
            inv2 = inv * inv
            masked = list(lead)
            masked[hk] = jnp.where(row_id > rk, lead[hk], 0.0)
            m = [None if x is None else x * inv2 for x in masked]
            for j in range(k + 1, size):
                hj, rj = j // 8, j % 8
                x = spread(lead[hj], rj)
                for h in range(hj, tiles):
                    step = (masked[h] * x) * inv2 if j == k + 1 else m[h] * x
                    cols[j][h] = cols[j][h] - step
            top = rows[hk][:, rk : rk + 1]
            for h in range(hk, tiles):
                rows[h] = rows[h] - along(m[h]) * top
            scale[hk] = jnp.where(row_id == rk, inv, scale[hk])
        rows = [x * along(s) for x, s in zip(rows, scale)]
        block = jnp.concatenate(rows, axis=1) if tiles > 1 else rows[0]
        for t in range(count):
            done[t].append(block[t][:, width:])
        if end < order:
            new = []
            for t in range(count):
                high = block[t].astype(BF16).astype(F32)
                low = block[t] - high
                left = [high[:, :width], low[:, :width], high[:, :width]]
                left = jnp.concatenate(left, axis=0).T[end:order].astype(BF16)
                right = jnp.concatenate([high, high, low], axis=0).astype(BF16)
                new.append(rest[t][size : order - start] - mm(left, right))
            rest = new
        start = end
    return [pad_rows(jnp.concatenate(d, axis=0), total) for d in done]


def orthonormal(bases, ranks, order, width):
    count = bases[0].shape[0]
    row = lax.broadcasted_iota(jnp.int32, (count, width), 0)
    col = lax.broadcasted_iota(jnp.int32, (count, width), 1)
    grams = []
    for basis, rank in zip(bases, ranks):
        high, low = split(basis)
        gram = stacked((high, low), (pad_rows(high, width), pad_rows(low, width)), 1)
        grams.append(gram + jnp.where((row == col) & (col >= rank), 1.0, 0.0))
    return whiten(grams, bases, order)


def basis_of(here, above, u, wide, rank):
    rows = here.shape[0]
    keep = lax.broadcasted_iota(jnp.int32, (rows, 2 * here.shape[1]), 0) < rank
    both = jnp.where(keep, jnp.concatenate([here, -above], axis=1), 0.0)
    return stacked(split(both), split(jnp.concatenate([u, wide], axis=1)), 1)


def backward(ortho, u, wide):
    back = stacked(split(ortho), split(jnp.concatenate([u, wide], axis=1)))
    width = u.shape[1]
    return jnp.concatenate([back[:, :width], -back[:, width:]], axis=1)


def new_right(back, v, up):
    width = v.shape[1]
    bh, bl = split(back)
    bh, bl = pad_rows(bh, width), pad_rows(bl, width)
    vh, vl = split(jnp.concatenate([v, up], axis=1))
    both = mm(vh, jnp.concatenate([bh, bl], axis=0), 1)
    return both[:, :width] + both[:, width:] + mm(vl, bh, 1)


class Piece:
    def __init__(self, own, ref, root, has, edges, send, recv, local=False):
        self.own, self.ref, self.root, self.has, self.edges = own, ref, root, has, edges
        self.send, self.recv, self.local = send, recv, local

    def copy(self, k, src):
        return pltpu.make_async_remote_copy(
            src_ref=src,
            dst_ref=self.ref,
            send_sem=self.send.at[k],
            recv_sem=self.recv,
            device_id=self.edges[k][1],
            device_id_type=MESH,
        )

    def send_all(self, src):
        for k, (cond, _) in enumerate(self.edges):
            @pl.when(cond)
            def _(k=k):
                self.copy(k, src).start()

    def begin(self, only=None):
        @pl.when(self.root if only is None else self.root & only)
        def _():
            self.send_all(self.own)
            if self.local:
                pltpu.make_async_copy(self.own, self.ref, self.recv).start()

    def forward(self, only=None):
        both = lambda cond: cond if only is None else cond & only
        if self.local:
            @pl.when(both(self.root))
            def _():
                pltpu.make_async_copy(self.ref, self.ref, self.recv).wait()

        @pl.when(both(self.has))
        def _():
            pltpu.make_async_copy(self.ref, self.ref, self.recv).wait()
            self.send_all(self.ref)

    def finish(self):
        @pl.when(self.root | self.has)
        def _():
            for k, (cond, _) in enumerate(self.edges):
                @pl.when(cond)
                def _(k=k):
                    self.copy(k, self.ref).wait_send()


def greet_all(n_row, n_col, r, c):
    barrier = pltpu.get_barrier_semaphore()
    for d in range(1, n_row):
        pl.semaphore_signal(barrier, inc=1, device_id=((r + d) % n_row, c), device_id_type=MESH)
    for d in range(1, n_col):
        pl.semaphore_signal(barrier, inc=1, device_id=(r, (c + d) % n_col), device_id_type=MESH)
    pl.semaphore_wait(barrier, n_row + n_col - 2)


def part(ref, lead, k, count):
    view = ref if lead is None else ref.at[lead]
    rows = view.shape[0] // count
    return view.at[pl.ds(k * rows, rows)]


def kernel(n_row, n_col, order_1, order_2, ranks, hu, hv, hnear, hsketch, out_u, out_v, *scratch):
    (
        u, v, near, sk, near_t, high, low, p_u, p_v, low_u, low_v, up_u, up_v, above_own, above,
        ex_u, ex_v, ex_w, wide, lower, u1, v1, u1t_own, above1_own, up1t, up1_v, above1,
        low1_u, low1_own, low1_t, send, recv, load,
    ) = scratch
    r, c = lax.axis_index("row"), lax.axis_index("col")
    height, width = u.shape[1:]
    far = 1.0 / (8.0 * height)
    rows_1, rows_2 = above.shape[1], above1.shape[1]
    two = range(2)
    level, side, levels = r // 2, r % 2, n_row // 2
    parity = c % 2
    pieces = []

    def piece(own, ref, root, has, edges, local=False):
        k = len(pieces)
        pieces.append(Piece(own, ref, root, has, edges, send.at[k], recv.at[k], local))
        return pieces[-1]

    other_row, other_col = r + 1 - 2 * side, c + 1 - 2 * parity
    spine = side == parity
    down_on = spine & (level + 1 < levels), (r + 2, c)
    down_over = spine & (level >= 1), (other_row, c)
    down_first = r == 0, (1, c)
    if levels > 1:
        beside = [
            ((r == 0) & (parity == 1), (1, c)),
            ((parity == 0) & (level == 1) & (side == 1), (r - 2, c)),
        ]
    else:
        beside = [down_first]

    def only(cond, edges):
        return [(a & cond, d) for a, d in edges]

    def down(own, ref, when, first):
        return piece(own, ref, (r == 0) & when, (r > 0) & when, only(when, [down_on, down_over] + first))

    def down_1(own, ref, on, when):
        at = side == on
        edges = [
            ((r == 1) & (on == 0), (0, c)),
            (at & (level + 1 < levels), (r + 2, c)),
            (at & (level >= 1), (other_row, c)),
        ]
        return piece(own, ref, (r == 1) & when, ((r > 1) | ((r == 0) & (on == 0))) & when, only(when, edges))

    def across(own, ref, source, when):
        at = parity == source % 2
        edges = [(at, (r, other_col)), (at & (c // 2 + 1 < n_col // 2), (r, c + 2))]
        return piece(own, ref, (c == source) & when, (c != source) & when, only(when, edges), True)

    def pivot(own, ref, k):
        mine = parity == k
        edges = only(mine, [down_first, ((r == 0) & (c + 2 < n_col), (0, c + 2)), down_on, down_over])
        edges.append((mine & (r > 0), (r, other_col)))
        root = (r == 0) & (c == 0)
        if k == 1:
            edges[1] = edges[1][0] | root, (0, jnp.where(root, 1, c + 2))
            edges[0] = edges[0][0] & jnp.logical_not(root), edges[0][1]
        has = jnp.where(mine, jnp.logical_not(root), r > 0)
        return piece(own, ref, root, has, edges)

    quarters, later_rows, always = range(4), r > 1, r >= 0
    pivots = [[pivot(part(a, 0, h, 4), part(b, None, h, 4), k) for h in quarters] for k, a, b in ((0, u, p_u), (1, v, p_v))]
    lows_v = [across(part(v, 0, h, 2), part(low_v, None, h, 2), 0, r > 0) for h in two]
    lows_u = [across(part(u, 0, h, 2), part(low_u, None, h, 2), 0, r > 0) for h in two]
    ups_u = [[down(part(u, t, h, 4), part(up_u, t, h, 4), c > 0 if t == 0 else always, beside if t else [down_first]) for h in quarters] for t in two]
    ups_a = [down(above_own, above, always, [down_first])]
    ups_v = [down(part(v, t, h, 4), part(up_v, t, h, 4), c > 0 if t == 0 else always, beside) for t in two for h in quarters]
    extras = [down_1(part(a, 0, h, 4), part(b, None, h, 4), 0, c == 1) for a, b in ((u, ex_u), (v, ex_v)) for h in quarters]
    extra_w = [down_1(part(wide, 0, h, 4), part(ex_w, None, h, 4), 0, c == 1) for h in quarters]
    chains_u = [
        down_1(part(u1t_own, t, h, 4), up1t.at[t].at[pl.ds(h * (rows_1 // 4), rows_1 // 4)], parity, c > 1 if t == 0 else always)
        for t in two
        for h in quarters
    ]
    chains_a = [down_1(above1_own, above1, parity, always)]
    chains_v = [down_1(part(v1, t, h, 2), part(up1_v, t, h, 2), parity, c > 1 if t == 0 else always) for t in two for h in two]
    lows1_u = [across(part(u1, 0, h, 2), part(low1_u, None, h, 2), 1, later_rows) for h in two]
    lows1_t = [across(part(low1_own, None, h, 2), part(low1_t, None, h, 2), 1, later_rows) for h in two]

    def begin(*groups, only=None):
        for g in groups:
            for x in g:
                x.begin(only)

    def forward(*groups, only=None):
        for g in groups:
            for x in g:
                x.forward(only)

    loads = [(hu, u), (hv, v), (hsketch, sk), (hnear, near)]
    copies = [pltpu.make_async_copy(a, b, load.at[k]) for k, (a, b) in enumerate(loads)]
    for x in copies:
        x.start()
    greet_all(n_row, n_col, r, c)
    for x in copies[:3]:
        x.wait()
    col_id = lax.broadcasted_iota(jnp.int32, (height, width), 1)
    for t in two:
        keep = col_id < ranks[0, 0, t, 0, r]
        u[t] = jnp.where(keep, u[t], 0.0)
        v[t] = jnp.where(keep, v[t], 0.0)
    begin(pivots[1], pivots[0], lows_v, lows_u, extras)
    sketch_t = [split(sk[k].T[:rows]) for k, rows in ((0, rows_1), (1, rows_2))]

    def here_of(v, k):
        both = stacked(sketch_t[k], split(jnp.concatenate([v[0], v[1]], axis=1)))
        return both[:, :width], both[:, width:]

    @pl.when(r == 0)
    def _():
        for t in two:
            begin(ups_u[t], only=parity != t)
        forward(pivots[0], pivots[1])
        for t in two:
            begin(ups_u[t], only=parity == t)
        a, b = here_of(v, 0)
        above_own[0] = a
        above_own[1] = b
        begin(ups_a, ups_v)
        copies[3].wait()
        for t in two:
            stays = (c > 0) | (t > 0)
            out_u[t] = jnp.where(stays, u[t], 0.0)
            out_v[t] = jnp.where(stays, v[t], 0.0)
        forward(extras, extra_w, chains_u, chains_a, chains_v)

    @pl.when((r > 0) & (c == 0))
    def _():
        up_u[0] = jnp.zeros((height, width), F32)
        up_v[0] = jnp.zeros((height, width), F32)

    @pl.when(r > 0)
    def _():
        for t in two:
            up1t[t, rows_1:] = jnp.zeros((width - rows_1, height), F32)

        @pl.when(c < 2)
        def _():
            up1t[0, :rows_1] = jnp.zeros((rows_1, height), F32)
            up1_v[0] = jnp.zeros((height, width), F32)

        copies[3].wait()
        near_t[0] = near[0].T

        @pl.when((c == 1) & later_rows)
        def _():
            near_t[1] = near[1].T

        scale = diagonal_inverse(near[0])
        here = here_of(v, 0)
        last = level + 1 == levels
        relays = later_rows & jnp.logical_not(last) & (spine | ((level == 1) & (parity == 0)))
        ends = later_rows & jnp.logical_not(relays)
        odd = parity == 1
        prompt = relays & (parity == 0)
        middle = (odd & ((r == 1) | relays)) | (last & spine & (parity == 0))
        late = jnp.logical_not(prompt | middle)
        first_on = spine & jnp.logical_not(last) & ((level == 1) | (c != 1))
        soon = first_on & odd & (level == 1)
        passes = relays | ((r == 1) & (parity == 1))
        leads = lambda cond: [forward(ups_u[t], only=passes & (parity != t) & cond) for t in two]
        forward(extras, only=later_rows & (side == 0))
        leads(c >= 2)
        forward(lows_v, only=parity == 0)
        for k in two:
            forward(pivots[k], only=parity == k)
        leads(c < 2)
        forward(lows_u, only=parity == 0)
        forward(ups_u[0], ups_a, only=relays & (parity == 0))
        early = relays & (level == 1) & (parity == 0)
        forward(ups_v, only=early)
        forward(lows_v, only=odd)
        for k in two:
            forward(pivots[k], only=parity != k)
        pivot_t = near_t[0] + far * deep(split(p_v[...]), split(p_u[...]), 1)
        high[...], low[...] = split(pivot_t)
        def hook(k):
            for t in two:
                if k < 4:
                    forward(ups_u[t][k : k + 1], only=ends & (parity != t))
                else:
                    forward(ups_u[t][k - 4 : k - 3], only=ends & (parity == t))
            if 0 < k < 5:
                forward(ups_u[1][k - 1 : k], only=odd & jnp.logical_not(ends))

        hooks = {k: functools.partial(hook, k) for k in range(7)}
        lower[...] = apply_inverse(high, low, scale, low_v[...], hooks)
        hook(7)
        forward(ups_u[1], ups_u[0], only=(r == 1) & (parity == 0))
        forward(extras, only=later_rows & (side == 1))
        forward(extra_w, only=later_rows & (side == 0) & jnp.logical_not(last))
        forward(lows_u, only=odd)
        forward(ups_v, only=prompt & jnp.logical_not(early))
        core = far * stacked(
            split(lower[...].T), split(jnp.concatenate([up_u[0], up_u[1]], axis=1))
        )
        lane = lax.broadcasted_iota(jnp.int32, core.shape, 1)
        live = (lane < ranks[0, 0, 0, 0, 0]) | ((lane >= width) & (lane < width + ranks[0, 0, 1, 0, 0]))
        core = jnp.where(live, core, 0.0)
        both = deep(split(low_u[...]), split(core))
        wide[0] = both[:, :width]
        wide[1] = both[:, width:]
        begin(extra_w)
        forward(ups_a, only=odd | jnp.logical_not(relays))
        rank_1 = [ranks[1, 0, t, 0, r] for t in two]
        bases = [basis_of(here[t], above[t], u[t], wide[t], rank_1[t]) for t in two]
        bases = orthonormal(bases, rank_1, order_1, width)
        forward(ups_v, only=middle)
        forward(chains_u, only=later_rows & soon)
        forward(extra_w, only=later_rows & (side == 0) & last)
        orthos = orthonormal(bases, rank_1, order_1, width)
        root_order = math.sqrt(height)
        tile_col = [t * n_col + c for t in two]
        chosen = [(tile_col[t] > 0) & jnp.logical_not((r == 1) & (tile_col[t] == 1)) for t in two]
        for t in two:
            u1t_own[t] = orthos[t] * root_order
        begin(chains_u)

        def set_left():
            for t in two:
                u1[t] = jnp.where(chosen[t], pad_rows(u1t_own[t], width).T, u[t])

        pl.when(later_rows)(set_left)
        begin(lows1_u)
        forward(chains_u, only=later_rows & first_on & jnp.logical_not(soon))

        def right_of(t):
            right = new_right(backward(orthos[t], u[t], wide[t]), v[t], up_v[t]) * (1.0 / root_order)
            return jnp.where(chosen[t], right, jnp.where(tile_col[t] == 0, lower[...], v[t]))

        forward(ups_v[:4], only=late)
        v1[0] = right_of(0)

        @pl.when((c == 1) & later_rows)
        def _():
            forward(extra_w, only=side == 1)
            left = jnp.concatenate([ex_v[...], up_v[0]], axis=1)
            right = jnp.concatenate([ex_u[...], -ex_w[...]], axis=1)
            lh, ll = split(left)
            rh, rl = split(right)
            pivot_t = near_t[1] + far * (mm(lh, rh, 1) + (mm(lh, rl, 1) + mm(ll, rh, 1)))
            high[...], low[...] = split(pivot_t)
            lower[...] = apply_inverse(high, low, diagonal_inverse(near[1]), v1[0], {})
            low1_own[...] = lower[...].T[:rows_1]

        begin(lows1_t)
        forward(ups_v[4:], only=late)
        v1[1] = right_of(1)
        here = here_of(v1, 1)
        above1_own[0] = here[0]
        above1_own[1] = here[1]
        begin(chains_a, chains_v)

        @pl.when(r == 1)
        def _():
            set_left()
            out_u[...] = u1[...]
            out_v[...] = v1[...]

        @pl.when(later_rows)
        def _():
            forward(lows1_u, only=odd)
            forward(chains_u, only=jnp.logical_not(first_on))
            forward(chains_a)
            forward(lows1_t, only=odd)
            forward(chains_v, only=spine & jnp.logical_not(last & odd))
            forward(lows1_u, lows1_t, only=parity == 0)
            core = far * stacked(split(low1_t[...]), split(up1t[...].reshape(2 * width, height)), 1)
            both = deep(split(low1_u[...]), split(pad_rows(core, width)))
            wide[0] = both[:, :width]
            wide[1] = both[:, width:]
            rank_2 = [ranks[2, 0, t, 0, r] for t in two]
            bases = [basis_of(here[t], above1[t], u1[t], wide[t], rank_2[t]) for t in two]
            bases = orthonormal(bases, rank_2, order_2, width)
            forward(chains_v, only=spine & last & odd)
            orthos = orthonormal(bases, rank_2, order_2, width)
            forward(chains_v, only=jnp.logical_not(spine))
            for t in two:
                live = tile_col[t] > 1
                right = new_right(backward(orthos[t], u1[t], wide[t]), v1[t], up1_v[t]) * (1.0 / root_order)
                out_u[t] = jnp.where(live, pad_rows(orthos[t] * root_order, width).T, u1[t])
                out_v[t] = jnp.where(live, right, jnp.where(tile_col[t] == 1, lower[...], v1[t]))

    for x in pieces:
        x.finish()


def body(n_row, n_col, factor_u, factor_v, near_field, sketch, tile_ranks):
    tiles, height, width = factor_u.shape[2], factor_u.shape[4], factor_u.shape[5]
    u = factor_u.reshape(tiles, height, width)
    v = factor_v.reshape(tiles, height, width)
    ranks = jnp.transpose(tile_ranks, (0, 1, 3, 4, 2))
    pair, one = (tiles, height, width), (height, width)
    order_1 = width - max(1, width // 4)
    order_2 = order_1 - max(1, order_1 // 4)
    rows_1, rows_2 = -(-order_1 // 16) * 16, -(-order_2 // 16) * 16
    square = (height, height)
    f32 = lambda *shape: pltpu.VMEM(shape, F32)
    buffers = [f32(*s) for s in (pair, pair, (2,) + square, (2,) + one, (2,) + square)]
    buffers += [pltpu.VMEM(square, BF16)] * 2
    buffers += [f32(*s) for s in (one, one, one, one, pair, pair, (2, rows_1, width), (2, rows_1, width))]
    buffers += [f32(*s) for s in (one, one, one, pair, one, pair, pair, (2, rows_1, height), (2, rows_2, width))]
    buffers += [f32(*s) for s in ((2, width, height), pair, (2, rows_2, width), one, (rows_1, height), (rows_1, height))]
    pieces = 58
    any_spec = pl.BlockSpec(memory_space=pl.ANY)
    out_u, out_v = pl.pallas_call(
        functools.partial(kernel, n_row, n_col, order_1, order_2),
        out_shape=[jax.ShapeDtypeStruct(pair, F32)] * 2,
        in_specs=[pl.BlockSpec(memory_space=pltpu.SMEM)] + [any_spec] * 4,
        out_specs=[pl.BlockSpec(memory_space=pltpu.VMEM)] * 2,
        scratch_shapes=buffers
        + [
            pltpu.SemaphoreType.DMA((pieces, EDGES)),
            pltpu.SemaphoreType.DMA((pieces,)),
            pltpu.SemaphoreType.DMA((4,)),
        ],
        compiler_params=pltpu.CompilerParams(
            collective_id=0, has_side_effects=True, vmem_limit_bytes=60 * 1024 * 1024
        ),
    )(ranks, u, v, near_field, sketch)
    tile_col = jnp.arange(tiles, dtype=jnp.int32) * n_col + lax.axis_index("col")
    stays = jnp.logical_not((lax.axis_index("row") == 1) & (tile_col == 1))[:, None, None]
    out_u, out_v = jnp.where(stays, out_u, 0.0), jnp.where(stays, out_v, 0.0)
    shape_out = (1, 1, tiles, 1, height, width)
    return (out_u.reshape(shape_out), out_v.reshape(shape_out))


def solution(mesh):
    tile_spec = P(None, "row", None, "col", None, None)
    return jax.shard_map(
        functools.partial(body, mesh.shape["row"], mesh.shape["col"]),
        mesh=mesh,
        in_specs=(tile_spec, tile_spec, P(), P(), P(None, None, None, None, "col")),
        out_specs=(tile_spec, tile_spec),
        check_vma=False,
    )
```

```python
import functools
import math

import jax
import jax.numpy as jnp
from jax import lax
from jax.experimental import pallas as pl
from jax.experimental.pallas import tpu as pltpu
from jax.sharding import PartitionSpec as P

NS_STEPS = 3
BLOCK = 16
EDGES = 5
F32 = jnp.float32
BF16 = jnp.bfloat16
MESH = pl.DeviceIdType.MESH


def split(x):
    high = x.astype(BF16)
    return high, (x - high.astype(F32)).astype(BF16)


def mm(a, b, contract_b=0):
    return lax.dot_general(a, b, (((1,), (contract_b,)), ((), ())), preferred_element_type=F32)


def stacked(a, b, contract_b=0):
    ah, al = a
    bh, bl = b
    n = ah.shape[0]
    both = mm(jnp.concatenate([ah, al], axis=0), bh, contract_b)
    return both[:n] + both[n:] + mm(ah, bl, contract_b)


def deep(a, b, contract_b=0):
    ah, al = a
    bh, bl = b
    axis = contract_b
    return mm(jnp.concatenate([ah, al], axis=1), jnp.concatenate([bh, bh], axis=axis), contract_b) + mm(
        ah, bl, contract_b
    )


def pad_rows(x, n):
    if x.shape[0] == n:
        return x
    return jnp.concatenate([x, jnp.zeros((n - x.shape[0], x.shape[1]), x.dtype)], axis=0)


def apply_inverse(high, low, scale, w, hooks):
    n = w.shape[1]
    x = scale * w
    for step in range(2**NS_STEPS - 1):
        xh, xl = split(x)
        both = mm(high[...], jnp.concatenate([xh, xl], axis=1))
        x = x + scale * (w - (both[:, :n] + both[:, n:] + mm(low[...], xh)))
        if step in hooks:
            hooks[step]()
    return x


def diagonal_inverse(near):
    n = near.shape[0]
    eye = lax.broadcasted_iota(jnp.int32, (n, n), 0) == lax.broadcasted_iota(jnp.int32, (n, n), 1)
    return 1.0 / jnp.sum(jnp.where(eye, near, 0.0), axis=1, keepdims=True)


def spread(x, j):
    return jnp.broadcast_to(x[:, j : j + 1], x.shape)


def whiten(grams, rights, order):
    count, width = len(grams), grams[0].shape[1]
    total = grams[0].shape[0]
    rest = [jnp.concatenate([g, x], axis=1) for g, x in zip(grams, rights)]
    done = [[] for _ in grams]
    start = 0
    while start < order:
        size = min(BLOCK, order - start)
        end = start + size
        tiles = size // 8
        row_id = lax.broadcasted_iota(jnp.int32, (1, 8, width), 1)
        column = lambda x, h, j: jnp.broadcast_to(x[8 * h : 8 * h + 8, start + j : start + j + 1], (8, width))
        cols = [
            [None if h < j // 8 else jnp.stack([column(x, h, j) for x in rest]) for h in range(tiles)]
            for j in range(size)
        ]
        rows = [jnp.stack([x[8 * h : 8 * h + 8] for x in rest]) for h in range(tiles)]
        lanes = rows[0].shape[2] // width
        along = lambda m: jnp.concatenate([m] * lanes, axis=2)
        scale = [jnp.ones((count, 8, width), F32) for _ in range(tiles)]
        for k in range(size):
            hk, rk = k // 8, k % 8
            lead = cols[k]
            inv = lax.rsqrt(spread(lead[hk], rk))
            inv2 = inv * inv
            masked = list(lead)
            masked[hk] = jnp.where(row_id > rk, lead[hk], 0.0)
            m = [None if x is None else x * inv2 for x in masked]
            for j in range(k + 1, size):
                hj, rj = j // 8, j % 8
                x = spread(lead[hj], rj)
                for h in range(hj, tiles):
                    step = (masked[h] * x) * inv2 if j == k + 1 else m[h] * x
                    cols[j][h] = cols[j][h] - step
            top = rows[hk][:, rk : rk + 1]
            for h in range(hk, tiles):
                rows[h] = rows[h] - along(m[h]) * top
            scale[hk] = jnp.where(row_id == rk, inv, scale[hk])
        rows = [x * along(s) for x, s in zip(rows, scale)]
        block = jnp.concatenate(rows, axis=1) if tiles > 1 else rows[0]
        for t in range(count):
            done[t].append(block[t][:, width:])
        if end < order:
            new = []
            for t in range(count):
                high = block[t].astype(BF16).astype(F32)
                low = block[t] - high
                left = [high[:, :width], low[:, :width], high[:, :width]]
                left = jnp.concatenate(left, axis=0).T[end:order].astype(BF16)
                right = jnp.concatenate([high, high, low], axis=0).astype(BF16)
                new.append(rest[t][size : order - start] - mm(left, right))
            rest = new
        start = end
    return [pad_rows(jnp.concatenate(d, axis=0), total) for d in done]


def orthonormal(bases, ranks, order, width):
    count = bases[0].shape[0]
    row = lax.broadcasted_iota(jnp.int32, (count, width), 0)
    col = lax.broadcasted_iota(jnp.int32, (count, width), 1)
    grams = []
    for basis, rank in zip(bases, ranks):
        high, low = split(basis)
        gram = stacked((high, low), (pad_rows(high, width), pad_rows(low, width)), 1)
        grams.append(gram + jnp.where((row == col) & (col >= rank), 1.0, 0.0))
    return whiten(grams, bases, order)


def basis_of(here, above, u, wide, rank):
    rows = here.shape[0]
    keep = lax.broadcasted_iota(jnp.int32, (rows, 2 * here.shape[1]), 0) < rank
    both = jnp.where(keep, jnp.concatenate([here, -above], axis=1), 0.0)
    return stacked(split(both), split(jnp.concatenate([u, wide], axis=1)), 1)


def backward(ortho, u, wide):
    back = stacked(split(ortho), split(jnp.concatenate([u, wide], axis=1)))
    width = u.shape[1]
    return jnp.concatenate([back[:, :width], -back[:, width:]], axis=1)


def new_right(back, v, up):
    width = v.shape[1]
    bh, bl = split(back)
    bh, bl = pad_rows(bh, width), pad_rows(bl, width)
    vh, vl = split(jnp.concatenate([v, up], axis=1))
    both = mm(vh, jnp.concatenate([bh, bl], axis=0), 1)
    return both[:, :width] + both[:, width:] + mm(vl, bh, 1)


class Piece:
    def __init__(self, own, ref, root, has, edges, send, recv, local=False):
        self.own, self.ref, self.root, self.has, self.edges = own, ref, root, has, edges
        self.send, self.recv, self.local = send, recv, local

    def copy(self, k, src):
        return pltpu.make_async_remote_copy(
            src_ref=src,
            dst_ref=self.ref,
            send_sem=self.send.at[k],
            recv_sem=self.recv,
            device_id=self.edges[k][1],
            device_id_type=MESH,
        )

    def send_all(self, src):
        for k, (cond, _) in enumerate(self.edges):
            @pl.when(cond)
            def _(k=k):
                self.copy(k, src).start()

    def begin(self, only=None):
        @pl.when(self.root if only is None else self.root & only)
        def _():
            self.send_all(self.own)
            if self.local:
                pltpu.make_async_copy(self.own, self.ref, self.recv).start()

    def forward(self, only=None):
        both = lambda cond: cond if only is None else cond & only
        if self.local:
            @pl.when(both(self.root))
            def _():
                pltpu.make_async_copy(self.ref, self.ref, self.recv).wait()

        @pl.when(both(self.has))
        def _():
            pltpu.make_async_copy(self.ref, self.ref, self.recv).wait()
            self.send_all(self.ref)

    def finish(self):
        @pl.when(self.root | self.has)
        def _():
            for k, (cond, _) in enumerate(self.edges):
                @pl.when(cond)
                def _(k=k):
                    self.copy(k, self.ref).wait_send()


def greet_all(n_row, n_col, r, c):
    barrier = pltpu.get_barrier_semaphore()
    for d in range(1, n_row):
        pl.semaphore_signal(barrier, inc=1, device_id=((r + d) % n_row, c), device_id_type=MESH)
    for d in range(1, n_col):
        pl.semaphore_signal(barrier, inc=1, device_id=(r, (c + d) % n_col), device_id_type=MESH)
    pl.semaphore_wait(barrier, n_row + n_col - 2)


def part(ref, lead, k, count):
    view = ref if lead is None else ref.at[lead]
    rows = view.shape[0] // count
    return view.at[pl.ds(k * rows, rows)]


def kernel(n_row, n_col, order_1, order_2, ranks, hu, hv, hnear, hsketch, out_u, out_v, *scratch):
    (
        u, v, near, sk, near_t, high, low, p_u, p_v, low_u, low_v, up_u, up_v, above_own, above,
        ex_u, ex_v, ex_w, wide, lower, u1, v1, u1t_own, above1_own, up1t, up1_v, above1,
        low1_u, low1_own, low1_t, send, recv, load,
    ) = scratch
    r, c = lax.axis_index("row"), lax.axis_index("col")
    height, width = u.shape[1:]
    far = 1.0 / (8.0 * height)
    rows_1, rows_2 = above.shape[1], above1.shape[1]
    two = range(2)
    level, side, levels = r // 2, r % 2, n_row // 2
    parity = c % 2
    pieces = []

    def piece(own, ref, root, has, edges, local=False):
        k = len(pieces)
        pieces.append(Piece(own, ref, root, has, edges, send.at[k], recv.at[k], local))
        return pieces[-1]

    other_row, other_col = r + 1 - 2 * side, c + 1 - 2 * parity
    spine = side == parity
    down_on = spine & (level + 1 < levels), (r + 2, c)
    down_over = spine & (level >= 1), (other_row, c)
    down_first = r == 0, (1, c)
    if levels > 1:
        beside = [
            ((r == 0) & (parity == 1), (1, c)),
            ((parity == 0) & (level == 1) & (side == 1), (r - 2, c)),
        ]
    else:
        beside = [down_first]

    def only(cond, edges):
        return [(a & cond, d) for a, d in edges]

    def down(own, ref, when, first):
        return piece(own, ref, (r == 0) & when, (r > 0) & when, only(when, [down_on, down_over] + first))

    def down_1(own, ref, on, when):
        at = side == on
        edges = [
            ((r == 1) & (on == 0), (0, c)),
            (at & (level + 1 < levels), (r + 2, c)),
            (at & (level >= 1), (other_row, c)),
        ]
        return piece(own, ref, (r == 1) & when, ((r > 1) | ((r == 0) & (on == 0))) & when, only(when, edges))

    def across(own, ref, source, when):
        at = parity == source % 2
        edges = [(at, (r, other_col)), (at & (c // 2 + 1 < n_col // 2), (r, c + 2))]
        return piece(own, ref, (c == source) & when, (c != source) & when, only(when, edges), True)

    def pivot(own, ref, k):
        mine = parity == k
        edges = only(mine, [down_first, ((r == 0) & (c + 2 < n_col), (0, c + 2)), down_on, down_over])
        edges.append((mine & (r > 0), (r, other_col)))
        root = (r == 0) & (c == 0)
        if k == 1:
            edges[1] = edges[1][0] | root, (0, jnp.where(root, 1, c + 2))
            edges[0] = edges[0][0] & jnp.logical_not(root), edges[0][1]
        has = jnp.where(mine, jnp.logical_not(root), r > 0)
        return piece(own, ref, root, has, edges)

    quarters, later_rows, always = range(4), r > 1, r >= 0
    pivots = [[pivot(part(a, 0, h, 4), part(b, None, h, 4), k) for h in quarters] for k, a, b in ((0, u, p_u), (1, v, p_v))]
    lows_v = [across(part(v, 0, h, 2), part(low_v, None, h, 2), 0, r > 0) for h in two]
    lows_u = [across(part(u, 0, h, 2), part(low_u, None, h, 2), 0, r > 0) for h in two]
    ups_u = [[down(part(u, t, h, 4), part(up_u, t, h, 4), c > 0 if t == 0 else always, beside if t else [down_first]) for h in quarters] for t in two]
    ups_a = [down(above_own, above, always, [down_first])]
    ups_v = [down(part(v, t, h, 4), part(up_v, t, h, 4), c > 0 if t == 0 else always, beside) for t in two for h in quarters]
    extras = [down_1(part(a, 0, h, 4), part(b, None, h, 4), 0, c == 1) for a, b in ((u, ex_u), (v, ex_v)) for h in quarters]
    extra_w = [down_1(part(wide, 0, h, 4), part(ex_w, None, h, 4), 0, c == 1) for h in quarters]
    chains_u = [
        down_1(part(u1t_own, t, h, 4), up1t.at[t].at[pl.ds(h * (rows_1 // 4), rows_1 // 4)], parity, c > 1 if t == 0 else always)
        for t in two
        for h in quarters
    ]
    chains_a = [down_1(above1_own, above1, parity, always)]
    chains_v = [down_1(part(v1, t, h, 2), part(up1_v, t, h, 2), parity, c > 1 if t == 0 else always) for t in two for h in two]
    lows1_u = [across(part(u1, 0, h, 2), part(low1_u, None, h, 2), 1, later_rows) for h in two]
    lows1_t = [across(part(low1_own, None, h, 2), part(low1_t, None, h, 2), 1, later_rows) for h in two]

    def begin(*groups, only=None):
        for g in groups:
            for x in g:
                x.begin(only)

    def forward(*groups, only=None):
        for g in groups:
            for x in g:
                x.forward(only)

    loads = [(hu, u), (hv, v), (hsketch, sk), (hnear, near)]
    copies = [pltpu.make_async_copy(a, b, load.at[k]) for k, (a, b) in enumerate(loads)]
    for x in copies:
        x.start()
    greet_all(n_row, n_col, r, c)
    for x in copies[:3]:
        x.wait()
    col_id = lax.broadcasted_iota(jnp.int32, (height, width), 1)
    for t in two:
        keep = col_id < ranks[0, 0, t, 0, r]
        u[t] = jnp.where(keep, u[t], 0.0)
        v[t] = jnp.where(keep, v[t], 0.0)
    begin(pivots[1], pivots[0], lows_v, lows_u, extras)
    sketch_t = [split(sk[k].T[:rows]) for k, rows in ((0, rows_1), (1, rows_2))]

    def here_of(v, k):
        both = stacked(sketch_t[k], split(jnp.concatenate([v[0], v[1]], axis=1)))
        return both[:, :width], both[:, width:]

    @pl.when(r == 0)
    def _():
        for t in two:
            begin(ups_u[t], only=parity != t)
        forward(pivots[0], pivots[1])
        for t in two:
            begin(ups_u[t], only=parity == t)
        a, b = here_of(v, 0)
        above_own[0] = a
        above_own[1] = b
        begin(ups_a, ups_v)
        copies[3].wait()
        for t in two:
            stays = (c > 0) | (t > 0)
            out_u[t] = jnp.where(stays, u[t], 0.0)
            out_v[t] = jnp.where(stays, v[t], 0.0)
        forward(extras, extra_w, chains_u, chains_a, chains_v)

    @pl.when((r > 0) & (c == 0))
    def _():
        up_u[0] = jnp.zeros((height, width), F32)
        up_v[0] = jnp.zeros((height, width), F32)

    @pl.when(r > 0)
    def _():
        for t in two:
            up1t[t, rows_1:] = jnp.zeros((width - rows_1, height), F32)

        @pl.when(c < 2)
        def _():
            up1t[0, :rows_1] = jnp.zeros((rows_1, height), F32)
            up1_v[0] = jnp.zeros((height, width), F32)

        copies[3].wait()
        near_t[0] = near[0].T

        @pl.when((c == 1) & later_rows)
        def _():
            near_t[1] = near[1].T

        scale = diagonal_inverse(near[0])
        here = here_of(v, 0)
        last = level + 1 == levels
        relays = later_rows & jnp.logical_not(last) & (spine | ((level == 1) & (parity == 0)))
        ends = later_rows & jnp.logical_not(relays)
        odd = parity == 1
        prompt = relays & (parity == 0)
        middle = (odd & ((r == 1) | relays)) | (last & spine & (parity == 0))
        late = jnp.logical_not(prompt | middle)
        first_on = spine & jnp.logical_not(last) & ((level == 1) | (c != 1))
        soon = first_on & odd & (level == 1)
        passes = relays | ((r == 1) & (parity == 1))
        leads = lambda cond: [forward(ups_u[t], only=passes & (parity != t) & cond) for t in two]
        forward(extras, only=later_rows & (side == 0))
        leads(c >= 2)
        forward(lows_v, only=parity == 0)
        for k in two:
            forward(pivots[k], only=parity == k)
        leads(c < 2)
        forward(lows_u, only=parity == 0)
        forward(ups_u[0], ups_a, only=relays & (parity == 0))
        early = relays & (level == 1) & (parity == 0)
        forward(ups_v, only=early)
        forward(lows_v, only=odd)
        for k in two:
            forward(pivots[k], only=parity != k)
        pivot_t = near_t[0] + far * deep(split(p_v[...]), split(p_u[...]), 1)
        high[...], low[...] = split(pivot_t)
        def hook(k):
            for t in two:
                if k < 4:
                    forward(ups_u[t][k : k + 1], only=ends & (parity != t))
                else:
                    forward(ups_u[t][k - 4 : k - 3], only=ends & (parity == t))
            if 0 < k < 5:
                forward(ups_u[1][k - 1 : k], only=odd & jnp.logical_not(ends))

        hooks = {k: functools.partial(hook, k) for k in range(7)}
        lower[...] = apply_inverse(high, low, scale, low_v[...], hooks)
        hook(7)
        forward(ups_u[1], ups_u[0], only=(r == 1) & (parity == 0))
        forward(extras, only=later_rows & (side == 1))
        forward(extra_w, only=later_rows & (side == 0) & jnp.logical_not(last))
        forward(lows_u, only=odd)
        forward(ups_v, only=prompt & jnp.logical_not(early))
        core = far * stacked(
            split(lower[...].T), split(jnp.concatenate([up_u[0], up_u[1]], axis=1))
        )
        lane = lax.broadcasted_iota(jnp.int32, core.shape, 1)
        live = (lane < ranks[0, 0, 0, 0, 0]) | ((lane >= width) & (lane < width + ranks[0, 0, 1, 0, 0]))
        core = jnp.where(live, core, 0.0)
        both = deep(split(low_u[...]), split(core))
        wide[0] = both[:, :width]
        wide[1] = both[:, width:]
        begin(extra_w)
        forward(ups_a, only=odd | jnp.logical_not(relays))
        rank_1 = [ranks[1, 0, t, 0, r] for t in two]
        bases = [basis_of(here[t], above[t], u[t], wide[t], rank_1[t]) for t in two]
        bases = orthonormal(bases, rank_1, order_1, width)
        forward(ups_v, only=middle)
        forward(chains_u, only=later_rows & soon)
        forward(extra_w, only=later_rows & (side == 0) & last)
        orthos = orthonormal(bases, rank_1, order_1, width)
        root_order = math.sqrt(height)
        tile_col = [t * n_col + c for t in two]
        chosen = [(tile_col[t] > 0) & jnp.logical_not((r == 1) & (tile_col[t] == 1)) for t in two]
        for t in two:
            u1t_own[t] = orthos[t] * root_order
        begin(chains_u)

        def set_left():
            for t in two:
                u1[t] = jnp.where(chosen[t], pad_rows(u1t_own[t], width).T, u[t])

        pl.when(later_rows)(set_left)
        begin(lows1_u)
        forward(chains_u, only=later_rows & first_on & jnp.logical_not(soon))

        def right_of(t):
            right = new_right(backward(orthos[t], u[t], wide[t]), v[t], up_v[t]) * (1.0 / root_order)
            return jnp.where(chosen[t], right, jnp.where(tile_col[t] == 0, lower[...], v[t]))

        forward(ups_v[:4], only=late)
        v1[0] = right_of(0)

        @pl.when((c == 1) & later_rows)
        def _():
            forward(extra_w, only=side == 1)
            left = jnp.concatenate([ex_v[...], up_v[0]], axis=1)
            right = jnp.concatenate([ex_u[...], -ex_w[...]], axis=1)
            lh, ll = split(left)
            rh, rl = split(right)
            pivot_t = near_t[1] + far * (mm(lh, rh, 1) + (mm(lh, rl, 1) + mm(ll, rh, 1)))
            high[...], low[...] = split(pivot_t)
            lower[...] = apply_inverse(high, low, diagonal_inverse(near[1]), v1[0], {})
            low1_own[...] = lower[...].T[:rows_1]

        begin(lows1_t)
        forward(ups_v[4:], only=late)
        v1[1] = right_of(1)
        here = here_of(v1, 1)
        above1_own[0] = here[0]
        above1_own[1] = here[1]
        begin(chains_a, chains_v)

        @pl.when(r == 1)
        def _():
            set_left()
            out_u[...] = u1[...]
            out_v[...] = v1[...]

        @pl.when(later_rows)
        def _():
            forward(lows1_u, only=odd)
            forward(chains_u, only=jnp.logical_not(first_on))
            forward(chains_a)
            forward(lows1_t, only=odd)
            forward(chains_v, only=spine & jnp.logical_not(last & odd))
            forward(lows1_u, lows1_t, only=parity == 0)
            core = far * stacked(split(low1_t[...]), split(up1t[...].reshape(2 * width, height)), 1)
            both = deep(split(low1_u[...]), split(pad_rows(core, width)))
            wide[0] = both[:, :width]
            wide[1] = both[:, width:]
            rank_2 = [ranks[2, 0, t, 0, r] for t in two]
            bases = [basis_of(here[t], above1[t], u1[t], wide[t], rank_2[t]) for t in two]
            bases = orthonormal(bases, rank_2, order_2, width)
            forward(chains_v, only=spine & last & odd)
            orthos = orthonormal(bases, rank_2, order_2, width)
            forward(chains_v, only=jnp.logical_not(spine))
            for t in two:
                live = tile_col[t] > 1
                right = new_right(backward(orthos[t], u1[t], wide[t]), v1[t], up1_v[t]) * (1.0 / root_order)
                out_u[t] = jnp.where(live, pad_rows(orthos[t] * root_order, width).T, u1[t])
                out_v[t] = jnp.where(live, right, jnp.where(tile_col[t] == 1, lower[...], v1[t]))

    for x in pieces:
        x.finish()


def body(n_row, n_col, factor_u, factor_v, near_field, sketch, tile_ranks):
    tiles, height, width = factor_u.shape[2], factor_u.shape[4], factor_u.shape[5]
    u = factor_u.reshape(tiles, height, width)
    v = factor_v.reshape(tiles, height, width)
    ranks = jnp.transpose(tile_ranks, (0, 1, 3, 4, 2))
    pair, one = (tiles, height, width), (height, width)
    order_1 = width - max(1, width // 4)
    order_2 = order_1 - max(1, order_1 // 4)
    rows_1, rows_2 = -(-order_1 // 16) * 16, -(-order_2 // 16) * 16
    square = (height, height)
    f32 = lambda *shape: pltpu.VMEM(shape, F32)
    buffers = [f32(*s) for s in (pair, pair, (2,) + square, (2,) + one, (2,) + square)]
    buffers += [pltpu.VMEM(square, BF16)] * 2
    buffers += [f32(*s) for s in (one, one, one, one, pair, pair, (2, rows_1, width), (2, rows_1, width))]
    buffers += [f32(*s) for s in (one, one, one, pair, one, pair, pair, (2, rows_1, height), (2, rows_2, width))]
    buffers += [f32(*s) for s in ((2, width, height), pair, (2, rows_2, width), one, (rows_1, height), (rows_1, height))]
    pieces = 58
    any_spec = pl.BlockSpec(memory_space=pl.ANY)
    out_u, out_v = pl.pallas_call(
        functools.partial(kernel, n_row, n_col, order_1, order_2),
        out_shape=[pltpu.VMEM(pair, F32)] * 2,
        in_specs=[pl.BlockSpec(memory_space=pltpu.SMEM)] + [any_spec] * 4,
        out_specs=[pl.BlockSpec(memory_space=pltpu.VMEM)] * 2,
        scratch_shapes=buffers
        + [
            pltpu.SemaphoreType.DMA((pieces, EDGES)),
            pltpu.SemaphoreType.DMA((pieces,)),
            pltpu.SemaphoreType.DMA((4,)),
        ],
        compiler_params=pltpu.CompilerParams(
            collective_id=0, has_side_effects=True, vmem_limit_bytes=60 * 1024 * 1024
        ),
    )(ranks, u, v, near_field, sketch)
    tile_col = jnp.arange(tiles, dtype=jnp.int32) * n_col + lax.axis_index("col")
    stays = jnp.logical_not((lax.axis_index("row") == 1) & (tile_col == 1))[:, None, None]
    out_u, out_v = jnp.where(stays, out_u, 0.0), jnp.where(stays, out_v, 0.0)
    shape_out = (1, 1, tiles, 1, height, width)
    return (out_u.reshape(shape_out), out_v.reshape(shape_out))


def solution(mesh):
    tile_spec = P(None, "row", None, "col", None, None)
    return jax.shard_map(
        functools.partial(body, mesh.shape["row"], mesh.shape["col"]),
        mesh=mesh,
        in_specs=(tile_spec, tile_spec, P(), P(), P(None, None, None, None, "col")),
        out_specs=(tile_spec, tile_spec),
        check_vma=False,
    )
```

```python
import functools
import math

import jax
import jax.numpy as jnp
from jax import lax
from jax.experimental import pallas as pl
from jax.experimental.pallas import tpu as pltpu
from jax.sharding import PartitionSpec as P

NS_STEPS = 3
BLOCK = 16
EDGES = 5
F32 = jnp.float32
BF16 = jnp.bfloat16
MESH = pl.DeviceIdType.MESH


def split(x):
    high = x.astype(BF16)
    return high, (x - high.astype(F32)).astype(BF16)


def mm(a, b, contract_b=0):
    return lax.dot_general(a, b, (((1,), (contract_b,)), ((), ())), preferred_element_type=F32)


def stacked(a, b, contract_b=0):
    ah, al = a
    bh, bl = b
    n = ah.shape[0]
    both = mm(jnp.concatenate([ah, al], axis=0), bh, contract_b)
    return both[:n] + both[n:] + mm(ah, bl, contract_b)


def deep(a, b, contract_b=0):
    ah, al = a
    bh, bl = b
    axis = contract_b
    return mm(jnp.concatenate([ah, al], axis=1), jnp.concatenate([bh, bh], axis=axis), contract_b) + mm(
        ah, bl, contract_b
    )


def pad_rows(x, n):
    if x.shape[0] == n:
        return x
    return jnp.concatenate([x, jnp.zeros((n - x.shape[0], x.shape[1]), x.dtype)], axis=0)


def apply_inverse(high, low, scale, w, hooks):
    n = w.shape[1]
    x = scale * w
    for step in range(2**NS_STEPS - 1):
        xh, xl = split(x)
        both = mm(high[...], jnp.concatenate([xh, xl], axis=1))
        x = x + scale * (w - (both[:, :n] + both[:, n:] + mm(low[...], xh)))
        if step in hooks:
            hooks[step]()
    return x


def diagonal_inverse(near):
    n = near.shape[0]
    eye = lax.broadcasted_iota(jnp.int32, (n, n), 0) == lax.broadcasted_iota(jnp.int32, (n, n), 1)
    return 1.0 / jnp.sum(jnp.where(eye, near, 0.0), axis=1, keepdims=True)


def spread(x, j):
    return jnp.broadcast_to(x[:, j : j + 1], x.shape)


def whiten(grams, rights, order):
    count, width = len(grams), grams[0].shape[1]
    total = grams[0].shape[0]
    rest = [jnp.concatenate([g, x], axis=1) for g, x in zip(grams, rights)]
    done = [[] for _ in grams]
    start = 0
    while start < order:
        size = min(BLOCK, order - start)
        end = start + size
        tiles = size // 8
        row_id = lax.broadcasted_iota(jnp.int32, (1, 8, width), 1)
        column = lambda x, h, j: jnp.broadcast_to(x[8 * h : 8 * h + 8, start + j : start + j + 1], (8, width))
        cols = [
            [None if h < j // 8 else jnp.stack([column(x, h, j) for x in rest]) for h in range(tiles)]
            for j in range(size)
        ]
        rows = [jnp.stack([x[8 * h : 8 * h + 8] for x in rest]) for h in range(tiles)]
        lanes = rows[0].shape[2] // width
        along = lambda m: jnp.concatenate([m] * lanes, axis=2)
        scale = [jnp.ones((count, 8, width), F32) for _ in range(tiles)]
        for k in range(size):
            hk, rk = k // 8, k % 8
            lead = cols[k]
            inv = lax.rsqrt(spread(lead[hk], rk))
            inv2 = inv * inv
            masked = list(lead)
            masked[hk] = jnp.where(row_id > rk, lead[hk], 0.0)
            m = [None if x is None else x * inv2 for x in masked]
            for j in range(k + 1, size):
                hj, rj = j // 8, j % 8
                x = spread(lead[hj], rj)
                for h in range(hj, tiles):
                    step = (masked[h] * x) * inv2 if j == k + 1 else m[h] * x
                    cols[j][h] = cols[j][h] - step
            top = rows[hk][:, rk : rk + 1]
            for h in range(hk, tiles):
                rows[h] = rows[h] - along(m[h]) * top
            scale[hk] = jnp.where(row_id == rk, inv, scale[hk])
        rows = [x * along(s) for x, s in zip(rows, scale)]
        block = jnp.concatenate(rows, axis=1) if tiles > 1 else rows[0]
        for t in range(count):
            done[t].append(block[t][:, width:])
        if end < order:
            new = []
            for t in range(count):
                high = block[t].astype(BF16).astype(F32)
                low = block[t] - high
                left = [high[:, :width], low[:, :width], high[:, :width]]
                left = jnp.concatenate(left, axis=0).T[end:order].astype(BF16)
                right = jnp.concatenate([high, high, low], axis=0).astype(BF16)
                new.append(rest[t][size : order - start] - mm(left, right))
            rest = new
        start = end
    return [pad_rows(jnp.concatenate(d, axis=0), total) for d in done]


def orthonormal(bases, ranks, order, width):
    count = bases[0].shape[0]
    row = lax.broadcasted_iota(jnp.int32, (count, width), 0)
    col = lax.broadcasted_iota(jnp.int32, (count, width), 1)
    grams = []
    for basis, rank in zip(bases, ranks):
        high, low = split(basis)
        gram = stacked((high, low), (pad_rows(high, width), pad_rows(low, width)), 1)
        grams.append(gram + jnp.where((row == col) & (col >= rank), 1.0, 0.0))
    return whiten(grams, bases, order)


def basis_of(here, above, u, wide, rank):
    rows = here.shape[0]
    keep = lax.broadcasted_iota(jnp.int32, (rows, 2 * here.shape[1]), 0) < rank
    both = jnp.where(keep, jnp.concatenate([here, -above], axis=1), 0.0)
    return stacked(split(both), split(jnp.concatenate([u, wide], axis=1)), 1)


def backward(ortho, u, wide):
    back = stacked(split(ortho), split(jnp.concatenate([u, wide], axis=1)))
    width = u.shape[1]
    return jnp.concatenate([back[:, :width], -back[:, width:]], axis=1)


def new_right(back, v, up):
    width = v.shape[1]
    bh, bl = split(back)
    bh, bl = pad_rows(bh, width), pad_rows(bl, width)
    vh, vl = split(jnp.concatenate([v, up], axis=1))
    both = mm(vh, jnp.concatenate([bh, bl], axis=0), 1)
    return both[:, :width] + both[:, width:] + mm(vl, bh, 1)


class Piece:
    def __init__(self, own, ref, root, has, edges, send, recv, local=False):
        self.own, self.ref, self.root, self.has, self.edges = own, ref, root, has, edges
        self.send, self.recv, self.local = send, recv, local

    def copy(self, k, src):
        return pltpu.make_async_remote_copy(
            src_ref=src,
            dst_ref=self.ref,
            send_sem=self.send.at[k],
            recv_sem=self.recv,
            device_id=self.edges[k][1],
            device_id_type=MESH,
        )

    def send_all(self, src):
        for k, (cond, _) in enumerate(self.edges):
            @pl.when(cond)
            def _(k=k):
                self.copy(k, src).start()

    def begin(self, only=None):
        @pl.when(self.root if only is None else self.root & only)
        def _():
            self.send_all(self.own)
            if self.local:
                pltpu.make_async_copy(self.own, self.ref, self.recv).start()

    def forward(self, only=None):
        both = lambda cond: cond if only is None else cond & only
        if self.local:
            @pl.when(both(self.root))
            def _():
                pltpu.make_async_copy(self.ref, self.ref, self.recv).wait()

        @pl.when(both(self.has))
        def _():
            pltpu.make_async_copy(self.ref, self.ref, self.recv).wait()
            self.send_all(self.ref)

    def finish(self):
        @pl.when(self.root | self.has)
        def _():
            for k, (cond, _) in enumerate(self.edges):
                @pl.when(cond)
                def _(k=k):
                    self.copy(k, self.ref).wait_send()


def greet_all(n_row, n_col, r, c):
    barrier = pltpu.get_barrier_semaphore()
    for d in range(1, n_row):
        pl.semaphore_signal(barrier, inc=1, device_id=((r + d) % n_row, c), device_id_type=MESH)
    for d in range(1, n_col):
        pl.semaphore_signal(barrier, inc=1, device_id=(r, (c + d) % n_col), device_id_type=MESH)
    pl.semaphore_wait(barrier, n_row + n_col - 2)


def part(ref, lead, k, count):
    view = ref if lead is None else ref.at[lead]
    rows = view.shape[0] // count
    return view.at[pl.ds(k * rows, rows)]


def kernel(n_row, n_col, order_1, order_2, ranks, hu, hv, hnear, hsketch, out_u, out_v, *scratch):
    (
        u, v, near, sk, near_t, high, low, p_u, p_v, low_u, low_v, up_u, up_v, above_own, above,
        ex_u, ex_v, ex_w, wide, lower, u1, v1, u1t_own, above1_own, up1t, up1_v, above1,
        low1_u, low1_own, low1_t, send, recv, load,
    ) = scratch
    r, c = lax.axis_index("row"), lax.axis_index("col")
    height, width = u.shape[1:]
    far = 1.0 / (8.0 * height)
    rows_1, rows_2 = above.shape[1], above1.shape[1]
    two = range(2)
    level, side, levels = r // 2, r % 2, n_row // 2
    parity = c % 2
    pieces = []

    def piece(own, ref, root, has, edges, local=False):
        k = len(pieces)
        pieces.append(Piece(own, ref, root, has, edges, send.at[k], recv.at[k], local))
        return pieces[-1]

    other_row, other_col = r + 1 - 2 * side, c + 1 - 2 * parity
    spine = side == parity
    down_on = spine & (level + 1 < levels), (r + 2, c)
    down_over = spine & (level >= 1), (other_row, c)
    down_first = r == 0, (1, c)
    if levels > 1:
        beside = [
            ((r == 0) & (parity == 1), (1, c)),
            ((parity == 0) & (level == 1) & (side == 1), (r - 2, c)),
        ]
    else:
        beside = [down_first]

    def only(cond, edges):
        return [(a & cond, d) for a, d in edges]

    def down(own, ref, when, first):
        return piece(own, ref, (r == 0) & when, (r > 0) & when, only(when, [down_on, down_over] + first))

    def down_1(own, ref, on, when):
        at = side == on
        edges = [
            ((r == 1) & (on == 0), (0, c)),
            (at & (level + 1 < levels), (r + 2, c)),
            (at & (level >= 1), (other_row, c)),
        ]
        return piece(own, ref, (r == 1) & when, ((r > 1) | ((r == 0) & (on == 0))) & when, only(when, edges))

    def across(own, ref, source, when):
        at = parity == source % 2
        edges = [(at, (r, other_col)), (at & (c // 2 + 1 < n_col // 2), (r, c + 2))]
        return piece(own, ref, (c == source) & when, (c != source) & when, only(when, edges), True)

    def pivot(own, ref, k):
        mine = parity == k
        edges = only(mine, [down_first, ((r == 0) & (c + 2 < n_col), (0, c + 2)), down_on, down_over])
        edges.append((mine & (r > 0), (r, other_col)))
        root = (r == 0) & (c == 0)
        if k == 1:
            edges[1] = edges[1][0] | root, (0, jnp.where(root, 1, c + 2))
            edges[0] = edges[0][0] & jnp.logical_not(root), edges[0][1]
        has = jnp.where(mine, jnp.logical_not(root), r > 0)
        return piece(own, ref, root, has, edges)

    quarters, later_rows, always = range(4), r > 1, r >= 0
    pivots = [[pivot(part(a, 0, h, 4), part(b, None, h, 4), k) for h in quarters] for k, a, b in ((0, u, p_u), (1, v, p_v))]
    lows_v = [across(part(v, 0, h, 2), part(low_v, None, h, 2), 0, r > 0) for h in two]
    lows_u = [across(part(u, 0, h, 2), part(low_u, None, h, 2), 0, r > 0) for h in two]
    ups_u = [[down(part(u, t, h, 4), part(up_u, t, h, 4), c > 0 if t == 0 else always, beside if t else [down_first]) for h in quarters] for t in two]
    ups_a = [down(above_own.at[t], above.at[t], always, [down_first]) for t in two]
    ups_v = [down(part(v, t, h, 4), part(up_v, t, h, 4), c > 0 if t == 0 else always, beside) for t in two for h in quarters]
    extras = [down_1(part(a, 0, h, 4), part(b, None, h, 4), 0, c == 1) for a, b in ((u, ex_u), (v, ex_v)) for h in quarters]
    extra_w = [down_1(part(wide, 0, h, 4), part(ex_w, None, h, 4), 0, c == 1) for h in quarters]
    chains_u = [
        down_1(part(u1t_own, t, h, 4), up1t.at[t].at[pl.ds(h * (rows_1 // 4), rows_1 // 4)], parity, c > 1 if t == 0 else always)
        for t in two
        for h in quarters
    ]
    chains_a = [down_1(above1_own.at[t], above1.at[t], parity, always) for t in two]
    chains_v = [down_1(part(v1, t, h, 4), part(up1_v, t, h, 4), parity, c > 1 if t == 0 else always) for t in two for h in quarters]
    lows1_u = [across(part(u1, 0, h, 2), part(low1_u, None, h, 2), 1, later_rows) for h in two]
    lows1_t = [across(part(low1_own, None, h, 2), part(low1_t, None, h, 2), 1, later_rows) for h in two]

    def begin(*groups, only=None):
        for g in groups:
            for x in g:
                x.begin(only)

    def forward(*groups, only=None):
        for g in groups:
            for x in g:
                x.forward(only)

    loads = [(hu, u), (hv, v), (hsketch, sk), (hnear, near)]
    copies = [pltpu.make_async_copy(a, b, load.at[k]) for k, (a, b) in enumerate(loads)]
    for x in copies:
        x.start()
    greet_all(n_row, n_col, r, c)
    for x in copies[:3]:
        x.wait()
    col_id = lax.broadcasted_iota(jnp.int32, (height, width), 1)
    for t in two:
        keep = col_id < ranks[0, 0, t, 0, r]
        u[t] = jnp.where(keep, u[t], 0.0)
        v[t] = jnp.where(keep, v[t], 0.0)
    begin(pivots[1], pivots[0], lows_v, lows_u, extras)
    sketch_t = [split(sk[k].T[:rows]) for k, rows in ((0, rows_1), (1, rows_2))]

    def here_of(v, k):
        both = stacked(sketch_t[k], split(jnp.concatenate([v[0], v[1]], axis=1)))
        return both[:, :width], both[:, width:]

    @pl.when(r == 0)
    def _():
        for t in two:
            begin(ups_u[t], only=parity != t)
        forward(pivots[0], pivots[1])
        for t in two:
            begin(ups_u[t], only=parity == t)
        a, b = here_of(v, 0)
        above_own[0] = a
        above_own[1] = b
        begin(ups_a, ups_v)
        copies[3].wait()
        for t in two:
            stays = (c > 0) | (t > 0)
            out_u[t] = jnp.where(stays, u[t], 0.0)
            out_v[t] = jnp.where(stays, v[t], 0.0)
        forward(extras, extra_w, chains_u, chains_a, chains_v)

    @pl.when((r > 0) & (c == 0))
    def _():
        up_u[0] = jnp.zeros((height, width), F32)
        up_v[0] = jnp.zeros((height, width), F32)

    @pl.when(r > 0)
    def _():
        for t in two:
            up1t[t, rows_1:] = jnp.zeros((width - rows_1, height), F32)

        @pl.when(c < 2)
        def _():
            up1t[0, :rows_1] = jnp.zeros((rows_1, height), F32)
            up1_v[0] = jnp.zeros((height, width), F32)

        copies[3].wait()
        near_t[0] = near[0].T

        @pl.when((c == 1) & later_rows)
        def _():
            near_t[1] = near[1].T

        scale = diagonal_inverse(near[0])
        here = here_of(v, 0)
        last = level + 1 == levels
        relays = later_rows & jnp.logical_not(last) & (spine | ((level == 1) & (parity == 0)))
        ends = later_rows & jnp.logical_not(relays)
        odd = parity == 1
        prompt = relays & (parity == 0)
        middle = (odd & ((r == 1) | relays)) | (last & spine & (parity == 0))
        late = jnp.logical_not(prompt | middle)
        first_on = spine & jnp.logical_not(last) & ((level == 1) | (c != 1))
        soon = first_on & odd & (level == 1)
        passes = relays | ((r == 1) & (parity == 1))
        leads = lambda cond: [forward(ups_u[t], only=passes & (parity != t) & cond) for t in two]
        forward(extras, only=later_rows & (side == 0))
        leads(c >= 2)
        forward(lows_v, only=parity == 0)
        for k in two:
            forward(pivots[k], only=parity == k)
        leads(c < 2)
        forward(lows_u, only=parity == 0)
        forward(ups_u[0], ups_a, only=relays & (parity == 0))
        early = relays & (level == 1) & (parity == 0)
        forward(ups_v, only=early)
        forward(lows_v, only=odd)
        for k in two:
            forward(pivots[k], only=parity != k)
        pivot_t = near_t[0] + far * deep(split(p_v[...]), split(p_u[...]), 1)
        high[...], low[...] = split(pivot_t)
        def hook(k):
            for t in two:
                if k < 4:
                    forward(ups_u[t][k : k + 1], only=ends & (parity != t))
                else:
                    forward(ups_u[t][k - 4 : k - 3], only=ends & (parity == t))
            if 0 < k < 5:
                forward(ups_u[1][k - 1 : k], only=odd & jnp.logical_not(ends))

        hooks = {k: functools.partial(hook, k) for k in range(7)}
        lower[...] = apply_inverse(high, low, scale, low_v[...], hooks)
        hook(7)
        forward(ups_u[1], ups_u[0], only=(r == 1) & (parity == 0))
        forward(extras, only=later_rows & (side == 1))
        forward(extra_w, only=later_rows & (side == 0) & jnp.logical_not(last))
        forward(lows_u, only=odd)
        forward(ups_v, only=prompt & jnp.logical_not(early))
        core = far * stacked(
            split(lower[...].T), split(jnp.concatenate([up_u[0], up_u[1]], axis=1))
        )
        lane = lax.broadcasted_iota(jnp.int32, core.shape, 1)
        live = (lane < ranks[0, 0, 0, 0, 0]) | ((lane >= width) & (lane < width + ranks[0, 0, 1, 0, 0]))
        core = jnp.where(live, core, 0.0)
        both = deep(split(low_u[...]), split(core))
        wide[0] = both[:, :width]
        wide[1] = both[:, width:]
        begin(extra_w)
        forward(ups_a, only=odd | jnp.logical_not(relays))
        rank_1 = [ranks[1, 0, t, 0, r] for t in two]
        bases = [basis_of(here[t], above[t], u[t], wide[t], rank_1[t]) for t in two]
        bases = orthonormal(bases, rank_1, order_1, width)
        forward(ups_v, only=middle)
        forward(chains_u, only=later_rows & soon)
        forward(extra_w, only=later_rows & (side == 0) & last)
        orthos = orthonormal(bases, rank_1, order_1, width)
        root_order = math.sqrt(height)
        tile_col = [t * n_col + c for t in two]
        chosen = [(tile_col[t] > 0) & jnp.logical_not((r == 1) & (tile_col[t] == 1)) for t in two]
        for t in two:
            u1t_own[t] = orthos[t] * root_order
        begin(chains_u)

        def set_left():
            for t in two:
                u1[t] = jnp.where(chosen[t], pad_rows(u1t_own[t], width).T, u[t])

        pl.when(later_rows)(set_left)
        begin(lows1_u)
        forward(chains_u, only=later_rows & first_on & jnp.logical_not(soon))

        def right_of(t):
            right = new_right(backward(orthos[t], u[t], wide[t]), v[t], up_v[t]) * (1.0 / root_order)
            return jnp.where(chosen[t], right, jnp.where(tile_col[t] == 0, lower[...], v[t]))

        forward(ups_v[:4], only=late)
        v1[0] = right_of(0)
        forward(ups_v[4:], only=late & spine)

        @pl.when((c == 1) & later_rows)
        def _():
            forward(extra_w, only=side == 1)
            left = jnp.concatenate([ex_v[...], up_v[0]], axis=1)
            right = jnp.concatenate([ex_u[...], -ex_w[...]], axis=1)
            lh, ll = split(left)
            rh, rl = split(right)
            pivot_t = near_t[1] + far * (mm(lh, rh, 1) + (mm(lh, rl, 1) + mm(ll, rh, 1)))
            high[...], low[...] = split(pivot_t)
            lower[...] = apply_inverse(high, low, diagonal_inverse(near[1]), v1[0], {})
            low1_own[...] = lower[...].T[:rows_1]

        begin(lows1_t)
        forward(ups_v[4:], only=late & jnp.logical_not(spine))
        v1[1] = right_of(1)
        here = here_of(v1, 1)
        above1_own[0] = here[0]
        above1_own[1] = here[1]
        begin(chains_a, chains_v)

        @pl.when(r == 1)
        def _():
            set_left()
            out_u[...] = u1[...]
            out_v[...] = v1[...]

        @pl.when(later_rows)
        def _():
            forward(lows1_u, only=odd)
            forward(chains_u, only=jnp.logical_not(first_on))
            forward(chains_a)
            forward(lows1_t, only=odd)
            forward(chains_v, only=spine & jnp.logical_not(last & odd))
            forward(lows1_u, lows1_t, only=parity == 0)
            core = far * stacked(split(low1_t[...]), split(up1t[...].reshape(2 * width, height)), 1)
            both = deep(split(low1_u[...]), split(pad_rows(core, width)))
            wide[0] = both[:, :width]
            wide[1] = both[:, width:]
            rank_2 = [ranks[2, 0, t, 0, r] for t in two]
            bases = [basis_of(here[t], above1[t], u1[t], wide[t], rank_2[t]) for t in two]
            bases = orthonormal(bases, rank_2, order_2, width)
            forward(chains_v, only=spine & last & odd)
            orthos = orthonormal(bases, rank_2, order_2, width)
            forward(chains_v, only=jnp.logical_not(spine))
            for t in two:
                live = tile_col[t] > 1
                right = new_right(backward(orthos[t], u1[t], wide[t]), v1[t], up1_v[t]) * (1.0 / root_order)
                out_u[t] = jnp.where(live, pad_rows(orthos[t] * root_order, width).T, u1[t])
                out_v[t] = jnp.where(live, right, jnp.where(tile_col[t] == 1, lower[...], v1[t]))

    for x in pieces:
        x.finish()


def body(n_row, n_col, factor_u, factor_v, near_field, sketch, tile_ranks):
    tiles, height, width = factor_u.shape[2], factor_u.shape[4], factor_u.shape[5]
    u = factor_u.reshape(tiles, height, width)
    v = factor_v.reshape(tiles, height, width)
    ranks = jnp.transpose(tile_ranks, (0, 1, 3, 4, 2))
    pair, one = (tiles, height, width), (height, width)
    order_1 = width - max(1, width // 4)
    order_2 = order_1 - max(1, order_1 // 4)
    rows_1, rows_2 = -(-order_1 // 16) * 16, -(-order_2 // 16) * 16
    square = (height, height)
    f32 = lambda *shape: pltpu.VMEM(shape, F32)
    buffers = [f32(*s) for s in (pair, pair, (2,) + square, (2,) + one, (2,) + square)]
    buffers += [pltpu.VMEM(square, BF16)] * 2
    buffers += [f32(*s) for s in (one, one, one, one, pair, pair, (2, rows_1, width), (2, rows_1, width))]
    buffers += [f32(*s) for s in (one, one, one, pair, one, pair, pair, (2, rows_1, height), (2, rows_2, width))]
    buffers += [f32(*s) for s in ((2, width, height), pair, (2, rows_2, width), one, (rows_1, height), (rows_1, height))]
    pieces = 64
    any_spec = pl.BlockSpec(memory_space=pl.ANY)
    out_u, out_v = pl.pallas_call(
        functools.partial(kernel, n_row, n_col, order_1, order_2),
        out_shape=[pltpu.VMEM(pair, F32)] * 2,
        in_specs=[pl.BlockSpec(memory_space=pltpu.SMEM)] + [any_spec] * 4,
        out_specs=[pl.BlockSpec(memory_space=pltpu.VMEM)] * 2,
        scratch_shapes=buffers
        + [
            pltpu.SemaphoreType.DMA((pieces, EDGES)),
            pltpu.SemaphoreType.DMA((pieces,)),
            pltpu.SemaphoreType.DMA((4,)),
        ],
        compiler_params=pltpu.CompilerParams(
            collective_id=0, has_side_effects=True, vmem_limit_bytes=60 * 1024 * 1024
        ),
    )(ranks, u, v, near_field, sketch)
    tile_col = jnp.arange(tiles, dtype=jnp.int32) * n_col + lax.axis_index("col")
    stays = jnp.logical_not((lax.axis_index("row") == 1) & (tile_col == 1))[:, None, None]
    out_u, out_v = jnp.where(stays, out_u, 0.0), jnp.where(stays, out_v, 0.0)
    shape_out = (1, 1, tiles, 1, height, width)
    return (out_u.reshape(shape_out), out_v.reshape(shape_out))


def solution(mesh):
    tile_spec = P(None, "row", None, "col", None, None)
    return jax.shard_map(
        functools.partial(body, mesh.shape["row"], mesh.shape["col"]),
        mesh=mesh,
        in_specs=(tile_spec, tile_spec, P(), P(), P(None, None, None, None, "col")),
        out_specs=(tile_spec, tile_spec),
        check_vma=False,
    )
```

```python
import functools
import math

import jax
import jax.numpy as jnp
from jax import lax
from jax.experimental import pallas as pl
from jax.experimental.pallas import tpu as pltpu
from jax.sharding import PartitionSpec as P

NS_STEPS = 3
BLOCK = 16
EDGES = 5
F32 = jnp.float32
BF16 = jnp.bfloat16
MESH = pl.DeviceIdType.MESH


def split(x):
    high = x.astype(BF16)
    return high, (x - high.astype(F32)).astype(BF16)


def mm(a, b, contract_b=0):
    return lax.dot_general(a, b, (((1,), (contract_b,)), ((), ())), preferred_element_type=F32)


def stacked(a, b, contract_b=0):
    ah, al = a
    bh, bl = b
    n = ah.shape[0]
    both = mm(jnp.concatenate([ah, al], axis=0), bh, contract_b)
    return both[:n] + both[n:] + mm(ah, bl, contract_b)


def deep(a, b, contract_b=0):
    ah, al = a
    bh, bl = b
    axis = contract_b
    return mm(jnp.concatenate([ah, al], axis=1), jnp.concatenate([bh, bh], axis=axis), contract_b) + mm(
        ah, bl, contract_b
    )


def pad_rows(x, n):
    if x.shape[0] == n:
        return x
    return jnp.concatenate([x, jnp.zeros((n - x.shape[0], x.shape[1]), x.dtype)], axis=0)


def apply_inverse(high, low, scale, w, hooks):
    n = w.shape[1]
    x = scale * w
    for step in range(2**NS_STEPS - 1):
        xh, xl = split(x)
        both = mm(high[...], jnp.concatenate([xh, xl], axis=1))
        x = x + scale * (w - (both[:, :n] + both[:, n:] + mm(low[...], xh)))
        if step in hooks:
            hooks[step]()
    return x


def diagonal_inverse(near):
    n = near.shape[0]
    eye = lax.broadcasted_iota(jnp.int32, (n, n), 0) == lax.broadcasted_iota(jnp.int32, (n, n), 1)
    return 1.0 / jnp.sum(jnp.where(eye, near, 0.0), axis=1, keepdims=True)


def spread(x, j):
    return jnp.broadcast_to(x[:, j : j + 1], x.shape)


def whiten(grams, rights, order):
    count, width = len(grams), grams[0].shape[1]
    total = grams[0].shape[0]
    rest = [jnp.concatenate([g, x], axis=1) for g, x in zip(grams, rights)]
    done = [[] for _ in grams]
    start = 0
    while start < order:
        size = min(BLOCK, order - start)
        end = start + size
        tiles = size // 8
        row_id = lax.broadcasted_iota(jnp.int32, (1, 8, width), 1)
        column = lambda x, h, j: jnp.broadcast_to(x[8 * h : 8 * h + 8, start + j : start + j + 1], (8, width))
        cols = [
            [None if h < j // 8 else jnp.stack([column(x, h, j) for x in rest]) for h in range(tiles)]
            for j in range(size)
        ]
        rows = [jnp.stack([x[8 * h : 8 * h + 8] for x in rest]) for h in range(tiles)]
        lanes = rows[0].shape[2] // width
        along = lambda m: jnp.concatenate([m] * lanes, axis=2)
        scale = [jnp.ones((count, 8, width), F32) for _ in range(tiles)]
        for k in range(size):
            hk, rk = k // 8, k % 8
            lead = cols[k]
            inv = lax.rsqrt(spread(lead[hk], rk))
            inv2 = inv * inv
            masked = list(lead)
            masked[hk] = jnp.where(row_id > rk, lead[hk], 0.0)
            m = [None if x is None else x * inv2 for x in masked]
            for j in range(k + 1, size):
                hj, rj = j // 8, j % 8
                x = spread(lead[hj], rj)
                for h in range(hj, tiles):
                    step = (masked[h] * x) * inv2 if j == k + 1 else m[h] * x
                    cols[j][h] = cols[j][h] - step
            top = rows[hk][:, rk : rk + 1]
            for h in range(hk, tiles):
                rows[h] = rows[h] - along(m[h]) * top
            scale[hk] = jnp.where(row_id == rk, inv, scale[hk])
        rows = [x * along(s) for x, s in zip(rows, scale)]
        block = jnp.concatenate(rows, axis=1) if tiles > 1 else rows[0]
        for t in range(count):
            done[t].append(block[t][:, width:])
        if end < order:
            new = []
            for t in range(count):
                high = block[t].astype(BF16).astype(F32)
                low = block[t] - high
                left = [high[:, :width], low[:, :width], high[:, :width]]
                left = jnp.concatenate(left, axis=0).T[end:order].astype(BF16)
                right = jnp.concatenate([high, high, low], axis=0).astype(BF16)
                new.append(rest[t][size : order - start] - mm(left, right))
            rest = new
        start = end
    return [pad_rows(jnp.concatenate(d, axis=0), total) for d in done]


def orthonormal(bases, ranks, order, width):
    count = bases[0].shape[0]
    row = lax.broadcasted_iota(jnp.int32, (count, width), 0)
    col = lax.broadcasted_iota(jnp.int32, (count, width), 1)
    grams = []
    for basis, rank in zip(bases, ranks):
        high, low = split(basis)
        gram = stacked((high, low), (pad_rows(high, width), pad_rows(low, width)), 1)
        grams.append(gram + jnp.where((row == col) & (col >= rank), 1.0, 0.0))
    return whiten(grams, bases, order)


def basis_of(here, above, u, wide, rank):
    rows = here.shape[0]
    keep = lax.broadcasted_iota(jnp.int32, (rows, 2 * here.shape[1]), 0) < rank
    both = jnp.where(keep, jnp.concatenate([here, -above], axis=1), 0.0)
    return stacked(split(both), split(jnp.concatenate([u, wide], axis=1)), 1)


def backward(ortho, u, wide):
    back = stacked(split(ortho), split(jnp.concatenate([u, wide], axis=1)))
    width = u.shape[1]
    return jnp.concatenate([back[:, :width], -back[:, width:]], axis=1)


def new_right(back, v, up):
    width = v.shape[1]
    bh, bl = split(back)
    bh, bl = pad_rows(bh, width), pad_rows(bl, width)
    vh, vl = split(jnp.concatenate([v, up], axis=1))
    both = mm(vh, jnp.concatenate([bh, bl], axis=0), 1)
    return both[:, :width] + both[:, width:] + mm(vl, bh, 1)


class Piece:
    def __init__(self, own, ref, root, has, edges, send, recv, local=False):
        self.own, self.ref, self.root, self.has, self.edges = own, ref, root, has, edges
        self.send, self.recv, self.local = send, recv, local

    def copy(self, k, src):
        return pltpu.make_async_remote_copy(
            src_ref=src,
            dst_ref=self.ref,
            send_sem=self.send.at[k],
            recv_sem=self.recv,
            device_id=self.edges[k][1],
            device_id_type=MESH,
        )

    def send_all(self, src):
        for k, (cond, _) in enumerate(self.edges):
            @pl.when(cond)
            def _(k=k):
                self.copy(k, src).start()

    def begin(self, only=None):
        @pl.when(self.root if only is None else self.root & only)
        def _():
            self.send_all(self.own)
            if self.local:
                pltpu.make_async_copy(self.own, self.ref, self.recv).start()

    def forward(self, only=None):
        both = lambda cond: cond if only is None else cond & only
        if self.local:
            @pl.when(both(self.root))
            def _():
                pltpu.make_async_copy(self.ref, self.ref, self.recv).wait()

        @pl.when(both(self.has))
        def _():
            pltpu.make_async_copy(self.ref, self.ref, self.recv).wait()
            self.send_all(self.ref)

    def finish(self):
        @pl.when(self.root | self.has)
        def _():
            for k, (cond, _) in enumerate(self.edges):
                @pl.when(cond)
                def _(k=k):
                    self.copy(k, self.ref).wait_send()


def greet_all(n_row, n_col, r, c):
    barrier = pltpu.get_barrier_semaphore()
    for d in range(1, n_row):
        pl.semaphore_signal(barrier, inc=1, device_id=((r + d) % n_row, c), device_id_type=MESH)
    for d in range(1, n_col):
        pl.semaphore_signal(barrier, inc=1, device_id=(r, (c + d) % n_col), device_id_type=MESH)
    pl.semaphore_wait(barrier, n_row + n_col - 2)


def part(ref, lead, k, count):
    view = ref if lead is None else ref.at[lead]
    rows = view.shape[0] // count
    return view.at[pl.ds(k * rows, rows)]


def kernel(n_row, n_col, order_1, order_2, ranks, hu, hv, hnear, hsketch, out_u, out_v, *scratch):
    (
        u, v, near, sk, near_t, high, low, p_u, p_v, low_u, low_v, up_u, up_v, above_own, above,
        ex_u, ex_v, ex_w, wide, lower, u1, v1, u1t_own, above1_own, up1t, up1_v, above1,
        low1_u, low1_own, low1_t, send, recv, load,
    ) = scratch
    r, c = lax.axis_index("row"), lax.axis_index("col")
    height, width = u.shape[1:]
    far = 1.0 / (8.0 * height)
    rows_1, rows_2 = above.shape[1], above1.shape[1]
    two = range(2)
    level, side, levels = r // 2, r % 2, n_row // 2
    parity = c % 2
    pieces = []

    def piece(own, ref, root, has, edges, local=False):
        k = len(pieces)
        pieces.append(Piece(own, ref, root, has, edges, send.at[k], recv.at[k], local))
        return pieces[-1]

    other_row, other_col = r + 1 - 2 * side, c + 1 - 2 * parity
    spine = side == parity
    down_on = spine & (level + 1 < levels), (r + 2, c)
    down_over = spine & (level >= 1), (other_row, c)
    down_first = r == 0, (1, c)
    if levels > 1:
        beside = [
            ((r == 0) & (parity == 1), (1, c)),
            ((parity == 0) & (level == 1) & (side == 1), (r - 2, c)),
        ]
    else:
        beside = [down_first]

    def only(cond, edges):
        return [(a & cond, d) for a, d in edges]

    def down(own, ref, when, first):
        return piece(own, ref, (r == 0) & when, (r > 0) & when, only(when, [down_on, down_over] + first))

    def down_1(own, ref, on, when):
        at = side == on
        edges = [
            ((r == 1) & (on == 0), (0, c)),
            (at & (level + 1 < levels), (r + 2, c)),
            (at & (level >= 1), (other_row, c)),
        ]
        return piece(own, ref, (r == 1) & when, ((r > 1) | ((r == 0) & (on == 0))) & when, only(when, edges))

    def across(own, ref, source, when):
        at = parity == source % 2
        edges = [(at, (r, other_col)), (at & (c // 2 + 1 < n_col // 2), (r, c + 2))]
        return piece(own, ref, (c == source) & when, (c != source) & when, only(when, edges), True)

    def pivot(own, ref, k):
        mine = parity == k
        edges = only(mine, [down_first, ((r == 0) & (c + 2 < n_col), (0, c + 2)), down_on, down_over])
        edges.append((mine & (r > 0), (r, other_col)))
        root = (r == 0) & (c == 0)
        if k == 1:
            edges[1] = edges[1][0] | root, (0, jnp.where(root, 1, c + 2))
            edges[0] = edges[0][0] & jnp.logical_not(root), edges[0][1]
        has = jnp.where(mine, jnp.logical_not(root), r > 0)
        return piece(own, ref, root, has, edges)

    quarters, later_rows, always = range(4), r > 1, r >= 0
    pivots = [[pivot(part(a, 0, h, 4), part(b, None, h, 4), k) for h in quarters] for k, a, b in ((0, u, p_u), (1, v, p_v))]
    lows_v = [across(part(v, 0, h, 2), part(low_v, None, h, 2), 0, r > 0) for h in two]
    lows_u = [across(part(u, 0, h, 2), part(low_u, None, h, 2), 0, r > 0) for h in two]
    ups_u = [[down(part(u, t, h, 4), part(up_u, t, h, 4), c > 0 if t == 0 else always, beside if t else [down_first]) for h in quarters] for t in two]
    ups_a = [down(above_own.at[t], above.at[t], always, [down_first]) for t in two]
    ups_v = [down(part(v, t, h, 4), part(up_v, t, h, 4), c > 0 if t == 0 else always, beside) for t in two for h in quarters]
    extras = [down_1(part(a, 0, h, 4), part(b, None, h, 4), 0, c == 1) for a, b in ((u, ex_u), (v, ex_v)) for h in quarters]
    extra_w = [down_1(part(wide, 0, h, 4), part(ex_w, None, h, 4), 0, c == 1) for h in quarters]
    chains_u = [
        down_1(part(u1t_own, t, h, 4), up1t.at[t].at[pl.ds(h * (rows_1 // 4), rows_1 // 4)], parity, c > 1 if t == 0 else always)
        for t in two
        for h in quarters
    ]
    chains_a = [down_1(above1_own.at[t], above1.at[t], parity, always) for t in two]
    chains_v = [down_1(part(v1, t, h, 4), part(up1_v, t, h, 4), parity, c > 1 if t == 0 else always) for t in two for h in quarters]
    lows1_u = [across(part(u1, 0, h, 2), part(low1_u, None, h, 2), 1, later_rows) for h in two]
    lows1_t = [across(part(low1_own, None, h, 2), part(low1_t, None, h, 2), 1, later_rows) for h in two]

    def begin(*groups, only=None):
        for g in groups:
            for x in g:
                x.begin(only)

    def forward(*groups, only=None):
        for g in groups:
            for x in g:
                x.forward(only)

    loads = [(hu, u), (hv, v), (hsketch, sk), (hnear, near)]
    copies = [pltpu.make_async_copy(a, b, load.at[k]) for k, (a, b) in enumerate(loads)]
    for x in copies:
        x.start()
    greet_all(n_row, n_col, r, c)
    for x in copies[:3]:
        x.wait()
    col_id = lax.broadcasted_iota(jnp.int32, (height, width), 1)
    for t in two:
        keep = col_id < ranks[0, 0, t, 0, r]
        u[t] = jnp.where(keep, u[t], 0.0)
        v[t] = jnp.where(keep, v[t], 0.0)
    begin(pivots[1], pivots[0], lows_v, lows_u, extras)
    sketch_t = [split(sk[k].T[:rows]) for k, rows in ((0, rows_1), (1, rows_2))]

    def here_of(v, k):
        both = stacked(sketch_t[k], split(jnp.concatenate([v[0], v[1]], axis=1)))
        return both[:, :width], both[:, width:]

    @pl.when(r == 0)
    def _():
        for t in two:
            begin(ups_u[t], only=parity != t)
        forward(pivots[0], pivots[1])
        for t in two:
            begin(ups_u[t], only=parity == t)
        a, b = here_of(v, 0)
        above_own[0] = a
        above_own[1] = b
        begin(ups_a, ups_v)
        copies[3].wait()
        for t in two:
            stays = (c > 0) | (t > 0)
            out_u[t] = jnp.where(stays, u[t], 0.0)
            out_v[t] = jnp.where(stays, v[t], 0.0)
        forward(extras, extra_w, chains_u, chains_a, chains_v)

    @pl.when((r > 0) & (c == 0))
    def _():
        up_u[0] = jnp.zeros((height, width), F32)
        up_v[0] = jnp.zeros((height, width), F32)

    @pl.when(r > 0)
    def _():
        for t in two:
            up1t[t, rows_1:] = jnp.zeros((width - rows_1, height), F32)

        @pl.when(c < 2)
        def _():
            up1t[0, :rows_1] = jnp.zeros((rows_1, height), F32)
            up1_v[0] = jnp.zeros((height, width), F32)

        copies[3].wait()
        near_t[0] = near[0].T

        @pl.when((c == 1) & later_rows)
        def _():
            near_t[1] = near[1].T

        scale = diagonal_inverse(near[0])
        here = here_of(v, 0)
        last = level + 1 == levels
        relays = later_rows & jnp.logical_not(last) & (spine | ((level == 1) & (parity == 0)))
        ends = later_rows & jnp.logical_not(relays)
        odd = parity == 1
        prompt = relays & (parity == 0)
        middle = (odd & ((r == 1) | relays)) | (last & spine & (parity == 0))
        late = jnp.logical_not(prompt | middle)
        first_on = spine & jnp.logical_not(last) & ((level == 1) | (c != 1))
        soon = first_on & odd & (level == 1)
        passes = relays | ((r == 1) & (parity == 1))
        leads = lambda cond: [forward(ups_u[t], only=passes & (parity != t) & cond) for t in two]
        forward(extras, only=later_rows & (side == 0))
        leads(c >= 2)
        forward(lows_v, only=parity == 0)
        for k in two:
            forward(pivots[k], only=parity == k)
        leads(c < 2)
        forward(lows_u, only=parity == 0)
        forward(ups_u[0], ups_a, only=relays & (parity == 0))
        early = relays & (level == 1) & (parity == 0)
        forward(ups_v, only=early)
        forward(lows_v, only=odd)
        for k in two:
            forward(pivots[k], only=parity != k)
        pivot_t = near_t[0] + far * deep(split(p_v[...]), split(p_u[...]), 1)
        high[...], low[...] = split(pivot_t)
        def hook(k):
            for t in two:
                if k < 4:
                    forward(ups_u[t][k : k + 1], only=ends & (parity != t))
                else:
                    forward(ups_u[t][k - 4 : k - 3], only=ends & (parity == t))
            if 0 < k < 5:
                forward(ups_u[1][k - 1 : k], only=odd & jnp.logical_not(ends))

        hooks = {k: functools.partial(hook, k) for k in range(7)}
        lower[...] = apply_inverse(high, low, scale, low_v[...], hooks)
        hook(7)
        forward(ups_u[1], ups_u[0], only=(r == 1) & (parity == 0))
        forward(extras, only=later_rows & (side == 1))
        forward(extra_w, only=later_rows & (side == 0) & jnp.logical_not(last))
        forward(lows_u, only=odd)
        forward(ups_v, only=prompt & jnp.logical_not(early))
        core = far * stacked(
            split(lower[...].T), split(jnp.concatenate([up_u[0], up_u[1]], axis=1))
        )
        lane = lax.broadcasted_iota(jnp.int32, core.shape, 1)
        live = (lane < ranks[0, 0, 0, 0, 0]) | ((lane >= width) & (lane < width + ranks[0, 0, 1, 0, 0]))
        core = jnp.where(live, core, 0.0)
        both = deep(split(low_u[...]), split(core))
        wide[0] = both[:, :width]
        wide[1] = both[:, width:]
        begin(extra_w)
        forward(ups_a, only=odd | jnp.logical_not(relays))
        rank_1 = [ranks[1, 0, t, 0, r] for t in two]
        bases = [basis_of(here[t], above[t], u[t], wide[t], rank_1[t]) for t in two]
        bases = orthonormal(bases, rank_1, order_1, width)
        forward(ups_v, only=middle)
        forward(chains_u, only=later_rows & soon)
        forward(extra_w, only=later_rows & (side == 0) & last)
        orthos = orthonormal(bases, rank_1, order_1, width)
        root_order = math.sqrt(height)
        tile_col = [t * n_col + c for t in two]
        chosen = [(tile_col[t] > 0) & jnp.logical_not((r == 1) & (tile_col[t] == 1)) for t in two]
        for t in two:
            u1t_own[t] = orthos[t] * root_order
        begin(chains_u)

        def set_left():
            for t in two:
                u1[t] = jnp.where(chosen[t], pad_rows(u1t_own[t], width).T, u[t])

        pl.when(later_rows)(set_left)
        begin(lows1_u)
        forward(chains_u, only=later_rows & first_on & jnp.logical_not(soon))

        def right_of(t):
            right = new_right(backward(orthos[t], u[t], wide[t]), v[t], up_v[t]) * (1.0 / root_order)
            return jnp.where(chosen[t], right, jnp.where(tile_col[t] == 0, lower[...], v[t]))

        forward(ups_v[:4], only=late)
        v1[0] = right_of(0)
        forward(ups_v[4:], only=late & spine)

        @pl.when((c == 1) & later_rows)
        def _():
            forward(extra_w, only=side == 1)
            left = jnp.concatenate([ex_v[...], up_v[0]], axis=1)
            right = jnp.concatenate([ex_u[...], -ex_w[...]], axis=1)
            lh, ll = split(left)
            rh, rl = split(right)
            pivot_t = near_t[1] + far * (mm(lh, rh, 1) + (mm(lh, rl, 1) + mm(ll, rh, 1)))
            high[...], low[...] = split(pivot_t)
            lower[...] = apply_inverse(high, low, diagonal_inverse(near[1]), v1[0], {})
            low1_own[...] = lower[...].T[:rows_1]

        begin(lows1_t)
        forward(ups_v[4:], only=late & jnp.logical_not(spine))
        v1[1] = right_of(1)
        here = here_of(v1, 1)
        above1_own[0] = here[0]
        above1_own[1] = here[1]
        begin(chains_a, chains_v)

        @pl.when(r == 1)
        def _():
            set_left()
            out_u[...] = u1[...]
            out_v[...] = v1[...]

        @pl.when(later_rows)
        def _():
            forward(lows1_u, only=odd)
            forward(chains_u, only=jnp.logical_not(first_on))
            forward(chains_a)
            nearest = spine & jnp.logical_not(last) & odd & (level == 1)
            forward(chains_v, only=nearest)
            forward(lows1_t, only=odd)
            forward(chains_v, only=spine & jnp.logical_not((last & odd) | nearest))
            forward(lows1_u, lows1_t, only=parity == 0)
            core = far * stacked(split(low1_t[...]), split(up1t[...].reshape(2 * width, height)), 1)
            both = deep(split(low1_u[...]), split(pad_rows(core, width)))
            wide[0] = both[:, :width]
            wide[1] = both[:, width:]
            rank_2 = [ranks[2, 0, t, 0, r] for t in two]
            bases = [basis_of(here[t], above1[t], u1[t], wide[t], rank_2[t]) for t in two]
            bases = orthonormal(bases, rank_2, order_2, width)
            forward(chains_v, only=spine & last & odd)
            orthos = orthonormal(bases, rank_2, order_2, width)
            forward(chains_v, only=jnp.logical_not(spine))
            for t in two:
                live = tile_col[t] > 1
                right = new_right(backward(orthos[t], u1[t], wide[t]), v1[t], up1_v[t]) * (1.0 / root_order)
                out_u[t] = jnp.where(live, pad_rows(orthos[t] * root_order, width).T, u1[t])
                out_v[t] = jnp.where(live, right, jnp.where(tile_col[t] == 1, lower[...], v1[t]))

    for x in pieces:
        x.finish()


def body(n_row, n_col, factor_u, factor_v, near_field, sketch, tile_ranks):
    tiles, height, width = factor_u.shape[2], factor_u.shape[4], factor_u.shape[5]
    u = factor_u.reshape(tiles, height, width)
    v = factor_v.reshape(tiles, height, width)
    ranks = jnp.transpose(tile_ranks, (0, 1, 3, 4, 2))
    pair, one = (tiles, height, width), (height, width)
    order_1 = width - max(1, width // 4)
    order_2 = order_1 - max(1, order_1 // 4)
    rows_1, rows_2 = -(-order_1 // 16) * 16, -(-order_2 // 16) * 16
    square = (height, height)
    f32 = lambda *shape: pltpu.VMEM(shape, F32)
    buffers = [f32(*s) for s in (pair, pair, (2,) + square, (2,) + one, (2,) + square)]
    buffers += [pltpu.VMEM(square, BF16)] * 2
    buffers += [f32(*s) for s in (one, one, one, one, pair, pair, (2, rows_1, width), (2, rows_1, width))]
    buffers += [f32(*s) for s in (one, one, one, pair, one, pair, pair, (2, rows_1, height), (2, rows_2, width))]
    buffers += [f32(*s) for s in ((2, width, height), pair, (2, rows_2, width), one, (rows_1, height), (rows_1, height))]
    pieces = 64
    any_spec = pl.BlockSpec(memory_space=pl.ANY)
    out_u, out_v = pl.pallas_call(
        functools.partial(kernel, n_row, n_col, order_1, order_2),
        out_shape=[pltpu.VMEM(pair, F32)] * 2,
        in_specs=[pl.BlockSpec(memory_space=pltpu.SMEM)] + [any_spec] * 4,
        out_specs=[pl.BlockSpec(memory_space=pltpu.VMEM)] * 2,
        scratch_shapes=buffers
        + [
            pltpu.SemaphoreType.DMA((pieces, EDGES)),
            pltpu.SemaphoreType.DMA((pieces,)),
            pltpu.SemaphoreType.DMA((4,)),
        ],
        compiler_params=pltpu.CompilerParams(
            collective_id=0, has_side_effects=True, vmem_limit_bytes=60 * 1024 * 1024
        ),
    )(ranks, u, v, near_field, sketch)
    tile_col = jnp.arange(tiles, dtype=jnp.int32) * n_col + lax.axis_index("col")
    stays = jnp.logical_not((lax.axis_index("row") == 1) & (tile_col == 1))[:, None, None]
    out_u, out_v = jnp.where(stays, out_u, 0.0), jnp.where(stays, out_v, 0.0)
    shape_out = (1, 1, tiles, 1, height, width)
    return (out_u.reshape(shape_out), out_v.reshape(shape_out))


def solution(mesh):
    tile_spec = P(None, "row", None, "col", None, None)
    return jax.shard_map(
        functools.partial(body, mesh.shape["row"], mesh.shape["col"]),
        mesh=mesh,
        in_specs=(tile_spec, tile_spec, P(), P(), P(None, None, None, None, "col")),
        out_specs=(tile_spec, tile_spec),
        check_vma=False,
    )
```
